256 devices in a mesh: expert: 32 (over x, z_lo, y), dp: 8 (over z_hi, core).
Axes of the slice: x: 4, y: 4, z: 8 (z_hi: 4, z_lo: 2; z = z_hi * 2 + z_lo), core: 2. Of those that a mesh axis runs over, the one named last changes fastest.
Arguments:
- tokens: bfloat16 [32768, 1440], P(('expert', 'dp')), may hold values from -6 to 6
- cotangent: bfloat16 [32768, 1440], P(('expert', 'dp')), may hold values from -0.3984375 to 0.3984375
- expert_ids: int32 [32768, 4], P(('expert', 'dp')), may hold values from 0 to 31, all different within a row; in each aligned block of 128 rows (0 to 127, 128 to 255, ...) at most 24 rows name the same one
- gate_weights: float32 [32768, 4], P(('expert', 'dp')), may hold values from 0.05 to 1
- w_gate: bfloat16 [32, 1440, 1440], P('expert', 'dp'), may hold values from -0.15625 to 0.15625
- w_up: bfloat16 [32, 1440, 1440], P('expert', 'dp'), may hold values from -0.15625 to 0.15625
- w_down: bfloat16 [32, 1440, 1440], P('expert', 'dp'), may hold values from -0.15625 to 0.15625
Outputs:
- mixed: bfloat16 [32768, 1440], P(('expert', 'dp'))
- grad_gate: bfloat16 [32, 1440, 1440], P('expert', 'dp')
- grad_up: bfloat16 [32, 1440, 1440], P('expert', 'dp')
- grad_down: bfloat16 [32, 1440, 1440], P('expert', 'dp')
The draws below stay inside these ranges and needn't reach their ends.
Inputs may be any that keep to these rules, and one draw needn't show every extreme that they name: `expert_ids`: each row names 4 different experts. Within the rows of one device no expert is named more than 24 times, a bound that some block reaches.
All inputs are finite; a program needn't handle non-finite values.
Results may differ from the reference program's by a relative error of at most 0.013.
Values may be sent and summed in bfloat16 or wider, within the bound.
A program may use at most 128 MiB of HBM per device.

```python
import math
import jax
import jax.numpy as jnp
import numpy as np
from jax import lax

D = 1440
FH = 1440
TOPK = 4
TOK_DEV = 128
CAP = 512
EXPERTS = 32
SLOT = 24
TOKENS = 32768
N_EXPERT = 32
N_DP = 8


def shard_levels(key, dims, pieces, smallest, high):
    level = 1.0
    for dim, shards_of in pieces:
        draws = jax.random.uniform(jax.random.fold_in(jax.random.fold_in(key, 6), dim), (shards_of,), jnp.float32, smallest / len(pieces), high / len(pieces))
        level = level * jnp.repeat(jnp.exp(draws), dims[dim] // shards_of).reshape((-1,) + (1,) * (len(dims) - 1 - dim))
    return level


def routed_block(stream_key, own, number, rows, number_of, top, reach, skew):
    ranking = jax.random.permutation(stream_key, number_of)
    packed, usual = shares(number_of, rows * top, reach, skew, True), shares(number_of, rows * top, reach, skew, False)
    places = jnp.arange(number_of)

    def named(sizes, offset_by):
        used = int((sizes > 0).sum())
        fixed = max(1, used // 4)
        shifted = fixed + (places - fixed + offset_by * (used - fixed)) % max(1, number_of - fixed)
        return jnp.zeros((number_of,), jnp.int32).at[ranking[jnp.where(places < fixed, places, shifted)]].set(jnp.asarray(sizes, jnp.int32))

    sizes = jnp.where(number % 4 == 0, named(packed, number // 4), named(usual, number - number // 4 - 1))
    mixed = jax.random.permutation(jax.random.fold_in(own, 3), number_of)
    giver, receiver = mixed[0:number_of // 2 * 2:2], mixed[1:number_of // 2 * 2:2]
    margin = jnp.minimum(sizes[giver] - 1, reach - sizes[receiver]) // 2
    margin = jnp.where((giver == ranking[0]) | (receiver == ranking[0]) | (sizes[receiver] == 0), 0, jnp.maximum(margin, 0))
    shifted = jax.random.randint(jax.random.fold_in(own, 4), (number_of // 2,), 0, 1 << 20) % (margin + 1)
    sizes = sizes.at[giver].add(-shifted).at[receiver].add(shifted)
    items = jnp.searchsorted(jnp.cumsum(sizes), jnp.arange(rows * top), side="right").astype(jnp.int32)
    listing = items.reshape(top, rows).T
    listing = listing[jax.random.permutation(jax.random.fold_in(own, 1), rows)]
    offset_by = jax.random.randint(jax.random.fold_in(own, 2), (rows, 1), 0, top)
    return jnp.take_along_axis(listing, (jnp.arange(top)[None, :] + offset_by) % top, axis=1)


def shares(count, total, bound, skew, full):
    weights = [(1 << 20) // math.isqrt(rank ** skew) + 1 for rank in range(1, count + 1)]
    largest = bound if full else min(bound, max(-(-total // count), total * weights[0] // sum(weights)))
    least = 1 if total - largest >= count - 1 else 0
    holding, rest = [largest] + [least] * (count - 1), total - largest - least * (count - 1)
    while rest > 0:
        candidates = [i for i in range(1, count) if holding[i] < largest] or [i for i in range(1, count) if holding[i] < bound]
        pool, left = sum([weights[i] for i in candidates]), rest
        for i in candidates:
            extra = min(bound - holding[i], max(1, left * weights[i] // pool), rest)
            holding[i] = holding[i] + extra
            rest = rest - extra
    return np.array(holding)


def centred(own_key, extent, scale, reach, split=(), kind=jnp.bfloat16):
    entries = scale * jax.random.normal(own_key, extent, jnp.float32)
    if split:
        entries = entries * shard_levels(own_key, extent, split, -0.22, 0.18)
    return jnp.clip(entries, -reach, reach).astype(kind)


def setup_inputs(seed: int = 0) -> dict:
    splits = jax.random.split(jax.random.key(seed), 8)
    tokens = centred(splits[0], (TOKENS, D), 1.0, 6.0, ((0, 256),))
    cotangent = centred(splits[1], (TOKENS, D), 0.05, 0.3984375, ((0, 256),))
    expert_ids_keys = jax.random.split(jax.random.fold_in(splits[2], 1), TOKENS // TOK_DEV)
    expert_ids_turns = jax.random.permutation(jax.random.fold_in(splits[2], 3), TOKENS // TOK_DEV)
    expert_ids = jax.vmap(lambda own, number: routed_block(jax.random.fold_in(splits[2], 2), own, number, TOK_DEV, EXPERTS, TOPK, SLOT, 2))(expert_ids_keys, expert_ids_turns).reshape((TOKENS, TOPK))
    gate_weights = jnp.clip(jnp.exp(math.log(1.0) - 2.9957323 * jax.random.uniform(splits[3], (TOKENS, TOPK), jnp.float32) ** shard_levels(splits[3], (TOKENS, TOPK), ((0, 256),), -0.2, 0.2)), 0.05, 1.0)
    w_gate = centred(splits[4], (EXPERTS, D, FH), D ** -0.5, 0.15625, ((0, 32), (1, 8)))
    w_up = centred(splits[5], (EXPERTS, D, FH), D ** -0.5, 0.15625, ((0, 32), (1, 8)))
    w_down = centred(splits[6], (EXPERTS, D, FH), FH ** -0.5, 0.15625, ((0, 32), (1, 8)))
    return dict(tokens=tokens, cotangent=cotangent, expert_ids=expert_ids, gate_weights=gate_weights, w_gate=w_gate, w_up=w_up, w_down=w_down)


SWISH_SLOPE = 1.702


def expert_pass(packed_x, packed_g, gate_mat, up_mat, down_mat):
    pre_gate = jnp.dot(packed_x, gate_mat, preferred_element_type=jnp.float32)
    pre_up = jnp.dot(packed_x, up_mat, preferred_element_type=jnp.float32)
    sigmoid_part = jax.nn.sigmoid(SWISH_SLOPE * pre_gate)
    value = pre_gate * sigmoid_part
    slope_term = sigmoid_part + SWISH_SLOPE * pre_gate * sigmoid_part * (1.0 - sigmoid_part)
    hidden = (value * (pre_up + 1.0)).astype(jnp.bfloat16)
    expert_out = jnp.dot(hidden, down_mat.T, preferred_element_type=jnp.float32).astype(jnp.bfloat16)
    d_hidden = jnp.dot(packed_g, down_mat, preferred_element_type=jnp.float32)
    grad_down = jnp.dot(packed_g.T, hidden, preferred_element_type=jnp.float32)
    d_gate = (d_hidden * (pre_up + 1.0) * slope_term).astype(jnp.bfloat16)
    d_up = (d_hidden * value).astype(jnp.bfloat16)
    grad_gate = jnp.dot(packed_x.T, d_gate, preferred_element_type=jnp.float32)
    grad_up = jnp.dot(packed_x.T, d_up, preferred_element_type=jnp.float32)
    return expert_out, jnp.stack([grad_gate, grad_up, grad_down]).astype(jnp.bfloat16)


def reference(tokens, cotangent, expert_ids, gate_weights, w_gate, w_up, w_down):
    assigns = TOK_DEV * TOPK
    expert_table = jnp.arange(EXPERTS, dtype=jnp.int32)

    def rank_block(block):
        onehot = (block[:, None] == expert_table[None, :]).astype(jnp.int32)
        local_rank = jnp.sum((jnp.cumsum(onehot, axis=0) - onehot) * onehot, axis=1)
        return local_rank, jnp.sum(onehot, axis=0)

    local_rank, block_counts = lax.map(rank_block, expert_ids.reshape(N_EXPERT * N_DP, assigns))
    local_rank = local_rank.reshape(N_EXPERT, N_DP, assigns)
    block_counts = block_counts.reshape(N_EXPERT, N_DP, EXPERTS)
    offsets = jnp.cumsum(block_counts, axis=0) - block_counts
    group_ids = expert_ids.reshape(N_EXPERT, N_DP, assigns)
    position = jnp.take_along_axis(offsets, group_ids, axis=2) + local_rank
    target = jnp.where(position < CAP, position, CAP).astype(jnp.int32)
    gates = gate_weights.reshape(N_EXPERT, N_DP, assigns)
    token_rows = tokens.reshape(N_EXPERT, N_DP, TOK_DEV, D)
    cot_rows = cotangent.reshape(N_EXPERT, N_DP, TOK_DEV, D)
    inputs = (jnp.swapaxes(group_ids, 0, 1), jnp.swapaxes(target, 0, 1), jnp.swapaxes(gates, 0, 1),
              jnp.swapaxes(token_rows, 0, 1), jnp.swapaxes(cot_rows, 0, 1))

    def run_expert(item):
        return expert_pass(item[0], item[1], item[2], item[3], item[4])

    def per_group(totals, group):
        ids_here, target_here, gates_here, tokens_here, cot_here = group
        token_copies = jnp.repeat(tokens_here, TOPK, axis=1)
        gated = (gates_here[:, :, None] * jnp.repeat(cot_here, TOPK, axis=1).astype(jnp.float32)).astype(jnp.bfloat16)
        packed_x = jnp.zeros((EXPERTS, CAP, D), jnp.bfloat16).at[ids_here, target_here].set(token_copies, mode="drop")
        packed_g = jnp.zeros((EXPERTS, CAP, D), jnp.bfloat16).at[ids_here, target_here].set(gated, mode="drop")
        outputs, group_grads = lax.map(run_expert, (packed_x, packed_g, w_gate, w_up, w_down))
        group_grads = lax.optimization_barrier(group_grads)
        totals = totals + group_grads.astype(jnp.float32)
        kept = (target_here < CAP).astype(jnp.float32)
        fetched = outputs[ids_here, jnp.minimum(target_here, CAP - 1)]
        weighted = (gates_here * kept)[:, :, None] * fetched.astype(jnp.float32)
        mixed_group = jnp.sum(weighted.reshape(N_EXPERT, TOK_DEV, TOPK, D), axis=2).astype(jnp.bfloat16)
        return totals, mixed_group

    totals = jnp.zeros((EXPERTS, 3, D, FH), jnp.float32)
    totals, mixed_all = lax.scan(per_group, totals, inputs)
    mixed = jnp.swapaxes(mixed_all, 0, 1).reshape(TOKENS, D)
    grads = totals.astype(jnp.bfloat16)
    return (mixed, grads[:, 0], grads[:, 1], grads[:, 2])
```

```python
import functools

import jax
import jax.numpy as jnp
from jax import lax
from jax.experimental import pallas as pl
from jax.experimental.pallas import tpu as pltpu
from jax.sharding import PartitionSpec as P

MESH = pl.DeviceIdType.MESH
SWISH_SLOPE = 1.702
F32, BF16 = jnp.float32, jnp.bfloat16
TOK = 128
CAP = 512
SLOT = 24
D = 1440
FH = 1440
OWN = 180
SENT = 184
CHUNK = 192
DP = 8 * CHUNK
PAIR = 2 * CHUNK
HALF = 96
SLOTS = 32 * SLOT
PLANE = 16 * SLOT
VM = functools.partial(pl.BlockSpec, memory_space=pltpu.VMEM)


def mul(value, k):
    return pl.multiple_of(value, k)


class Place:
    def __init__(self):
        e, d = lax.axis_index("expert"), lax.axis_index("dp")
        self.x, self.zl, self.y = e // 8, (e // 4) % 2, e % 4
        self.h, self.c = d // 2, d % 2
        self.e, self.d = e, d
        self.sibling = (e, self.h * 2 + 1 - self.c)
        self.up = (e, ((self.h + 1) % 4) * 2 + self.c)
        self.down = (e, ((self.h + 3) % 4) * 2 + self.c)
        self.partner = (self.x * 8 + (1 - self.zl) * 4 + self.y, d)
        self.p = self.x * 4 + self.y

    def plane(self, i, sign):
        px = (self.x + sign * (i // 4) + 4) % 4
        py = (self.y + sign * (i % 4) + 4) % 4
        return px * 4 + py, px, py

    def plane_device(self, px, py):
        return (px * 8 + self.zl * 4 + py, self.d)

    def block(self, px, py, bi):
        zb = self.zl if bi == 0 else 1 - self.zl
        return px * 8 + zb * 4 + py

    def greet(self):
        barrier = pltpu.get_barrier_semaphore()
        for peer in (self.sibling, self.up, self.down, self.partner):
            pl.semaphore_signal(barrier, inc=1, device_id=peer, device_id_type=MESH)

        @pl.loop(1, 16)
        def _(i):
            _, px, py = self.plane(i, 1)
            pl.semaphore_signal(
                barrier, inc=1, device_id=self.plane_device(px, py), device_id_type=MESH
            )

        pl.semaphore_wait(barrier, 19)


def remote(src, dst, ssem, rsem, device):
    return pltpu.make_async_remote_copy(
        src_ref=src, dst_ref=dst, send_sem=ssem, recv_sem=rsem, device_id=device, device_id_type=MESH
    )


def rows_of(block, size=SLOT):
    return pl.ds(mul(block * SLOT, 8), size)


def dot(a, b):
    return jnp.dot(a, b, preferred_element_type=F32)


def dot_nt(a, b):
    return lax.dot_general(a, b, (((1,), (1,)), ((), ())), preferred_element_type=F32)


def dot_tn(a, b):
    return lax.dot_general(a, b, (((0,), (0,)), ((), ())), preferred_element_type=F32)


def one_zero(flag):
    return jnp.where(flag, 1.0, 0.0)


def gather_kernel(
    meta, tok, cot, wg_in, wu_in, wd_in,
    x_out, g_out, hid_out, dg_out, du_out, eo_out, r_out, mt_out,
    wg, wu, wd, zmeta, ztok, zcot, send_x, send_g, recv_x, recv_g, acc_g, acc_u, acc_d,
    loc_sem, zs, zr, ags, agr, ds_, dr,
):
    me = Place()
    h, c = me.h, me.c
    weights = (wg, wu, wd)

    def base(j, core):
        return CHUNK * (2 * j + core)

    def shard(w, j, core, lo=0, size=SENT):
        return w.at[pl.ds(mul(base(j, core) + lo, 8), size), :]

    own_copies = [
        pltpu.make_async_copy(
            src, w.at[pl.ds(mul(base(h, c), 8), SENT), :], loc_sem.at[a]
        )
        for a, (src, w) in enumerate(
            ((wg_in.at[pl.ds(0, SENT), :], wg), (wu_in.at[pl.ds(0, SENT), :], wu), (wd_in.at[pl.ds(0, SENT), :], wd))
        )
    ]
    for cp in own_copies:
        cp.start()
    for w in weights:
        for k in range(8):
            w[pl.ds(CHUNK * k + SENT, CHUNK - SENT), :] = jnp.zeros((CHUNK - SENT, FH), BF16)

    me.greet()

    zex = [
        remote(src, dst, zs.at[k], zr.at[k], me.partner)
        for k, (src, dst) in enumerate(((meta, zmeta), (tok, ztok), (cot, zcot)))
    ]
    for cp in zex:
        cp.start()

    def up_j(k):
        return (h + k) % 4

    def ag(a, k):
        w = weights[a]
        s, r = ags.at[a * 9 + k], agr.at[a * 9 + k]
        if k == 0:
            return remote(shard(w, h, c), shard(w, h, c), s, r, me.up)
        if k == 1:
            return remote(shard(w, h, c), shard(w, h, c), s, r, me.down)
        if k == 2:
            return remote(shard(w, h, c), shard(w, h, c), s, r, me.sibling)
        if k == 3:
            part = shard(w, up_j(3), c, 0, HALF)
            return remote(part, part, s, r, me.up)
        if k == 4:
            part = shard(w, up_j(1), c, HALF, SENT - HALF)
            return remote(part, part, s, r, me.down)
        if k in (5, 6):
            part = shard(w, up_j(3 if k == 5 else 1), c)
            return remote(part, part, s, r, me.sibling)
        part = shard(w, up_j(2), c, 0, HALF) if k == 7 else shard(w, up_j(2), c, HALF, SENT - HALF)
        return remote(part, part, s, r, me.sibling)

    def ag_in(a, k):
        w = weights[a]
        s, r = ags.at[a * 9 + k], agr.at[a * 9 + k]
        lo, size = 0, SENT
        if k == 0:
            j, core = up_j(3), c
        elif k == 1:
            j, core = up_j(1), c
        elif k == 2:
            j, core = h, 1 - c
        elif k == 3:
            j, core, size = up_j(2), c, HALF
        elif k == 4:
            j, core, lo, size = up_j(2), c, HALF, SENT - HALF
        elif k in (5, 6):
            j, core = up_j(3 if k == 5 else 1), 1 - c
        elif k == 7:
            j, core, size = up_j(2), 1 - c, HALF
        else:
            j, core, lo, size = up_j(2), 1 - c, HALF, SENT - HALF
        part = shard(w, j, core, lo, size)
        return remote(part, part, s, r, me.sibling)

    for a in (0, 1):
        own_copies[a].wait()
        for k in (0, 1, 2):
            ag(a, k).start()
    own_copies[2].wait()

    def dispatch_copy(bi, i, incoming):
        sign = -1 if incoming else 1
        p, px, py = me.plane(i, sign)
        at = (bi * 16 + p) * SLOT
        source = me.block(px, py, bi) if incoming else me.block(me.x, me.y, bi)
        copies = []
        for arr, (src, dst) in enumerate(((send_x, recv_x), (send_g, recv_g))):
            k = (bi * 2 + arr) * 16 + i
            copies.append(
                remote(
                    src.at[pl.ds(mul(at, 8), SLOT), :],
                    dst.at[rows_of(source), :],
                    ds_.at[k],
                    dr.at[k],
                    me.plane_device(px, py),
                )
            )
        return copies

    def dispatch(bi, m_ref, t_ref, c_ref):
        place = lax.broadcasted_iota(jnp.int32, (16, TOK), 0)
        expert = ((place // 4) * 8 + me.zl * 4 + place % 4).astype(F32)
        named = jnp.zeros((16, TOK), F32)
        gates = jnp.zeros((16, TOK), F32)
        for k in range(4):
            hit = m_ref[k : k + 1, :] == expert
            named = named + one_zero(hit)
            gates = gates + jnp.where(hit, m_ref[4 + k : 5 + k, :], 0.0)
        earlier = one_zero(
            lax.broadcasted_iota(jnp.int32, (TOK, TOK), 0) < lax.broadcasted_iota(jnp.int32, (TOK, TOK), 1)
        ).astype(BF16)
        rank = dot(named.astype(BF16), earlier)
        rank = jnp.where(named > 0.5, rank, -1.0)
        slot = lax.broadcasted_iota(jnp.int32, (16, SLOT, TOK), 1).astype(F32)
        chosen3 = one_zero(slot == rank[:, None, :])
        chosen = chosen3.reshape(PLANE, TOK)
        weighted = (chosen3 * gates[:, None, :]).reshape(PLANE, TOK)
        mt_out[bi] = weighted
        slot_gate = jnp.sum(weighted, axis=1, keepdims=True)
        pick = chosen.astype(BF16)
        send_x[pl.ds(bi * PLANE, PLANE), :] = dot(pick, t_ref[...]).astype(BF16)
        send_g[pl.ds(bi * PLANE, PLANE), :] = (dot(pick, c_ref[...]) * slot_gate).astype(BF16)
        mine = rows_of(me.block(me.x, me.y, bi))
        here = pl.ds(mul((bi * 16 + me.p) * SLOT, 8), SLOT)
        recv_x[mine, :] = send_x[here, :]
        recv_g[mine, :] = send_g[here, :]

        @pl.loop(1, 16)
        def _(i):
            for cp in dispatch_copy(bi, i, False):
                cp.start()

    dispatch(0, meta, tok, cot)
    for cp in zex:
        cp.wait_recv()
    dispatch(1, zmeta, ztok, zcot)

    def forward_neighbours(a):
        ag_in(a, 0).wait_recv()
        ag(a, 3).start()
        ag(a, 5).start()
        ag_in(a, 1).wait_recv()
        ag(a, 4).start()
        ag(a, 6).start()

    forward_neighbours(0)
    forward_neighbours(1)
    for k in (0, 1, 2):
        ag(2, k).start()

    for bi in range(2):

        @pl.loop(1, 16)
        def _(i):
            for cp in dispatch_copy(bi, i, True):
                cp.wait_recv()

    eye_lane = one_zero(lax.broadcasted_iota(jnp.int32, (8, 128), 1) == OWN - 128).astype(BF16)
    flags = dot_nt(eye_lane, recv_x[:, 128:256])
    before = one_zero(
        lax.broadcasted_iota(jnp.int32, (SLOTS, SLOTS), 0) < lax.broadcasted_iota(jnp.int32, (SLOTS, SLOTS), 1)
    ).astype(BF16)
    position = dot(flags.astype(BF16), before)
    position = jnp.where(flags > 0.5, position, -1.0)[0:1, :]

    @pl.loop(0, 2)
    def _(m):
        at = mul(m * 256, 256)
        row = (lax.broadcasted_iota(jnp.int32, (256, SLOTS), 0) + at).astype(F32)
        pick = one_zero(row == position).astype(BF16)
        r_out[pl.ds(at, 256), :] = pick
        x_out[pl.ds(at, 256), :] = dot(pick, recv_x[...]).astype(BF16)
        g_out[pl.ds(at, 256), :] = dot(pick, recv_g[...]).astype(BF16)

    def project(j, first):
        cols = pl.ds(mul(j * PAIR, 128), PAIR)

        @pl.loop(0, 2)
        def _(m):
            rows = pl.ds(mul(m * 256, 256), 256)
            xs = x_out[rows, cols]
            for acc, w in ((acc_g, wg), (acc_u, wu)):
                part = dot(xs, w[cols, :])
                acc[rows, :] = part if first else acc[rows, :] + part

    for a in (0, 1):
        ag_in(a, 2).wait_recv()
    project(h, True)
    for a in (0, 1):
        ag_in(a, 5).wait_recv()
    project(up_j(3), False)
    for a in (0, 1):
        ag_in(a, 6).wait_recv()
    project(up_j(1), False)

    def finish_gather(a):
        ag_in(a, 3).wait_recv()
        ag(a, 7).start()
        ag_in(a, 4).wait_recv()
        ag(a, 8).start()

    def wait_opposite(a):
        ag_in(a, 7).wait_recv()
        ag_in(a, 8).wait_recv()

    finish_gather(0)
    finish_gather(1)
    wait_opposite(0)
    wait_opposite(1)
    project(up_j(2), False)

    @pl.loop(0, 16)
    def _(m):
        rows = pl.ds(mul(m * 32, 32), 32)
        gate, up = acc_g[rows, :], acc_u[rows, :] + 1.0
        sg = jax.nn.sigmoid(SWISH_SLOPE * gate)
        value = gate * sg
        slope = sg + SWISH_SLOPE * value * (1.0 - sg)
        hid_out[rows, :] = (value * up).astype(BF16)
        acc_g[rows, :] = up * slope
        acc_u[rows, :] = value

    def down_step(j, first):
        cols = pl.ds(mul(j * PAIR, 128), PAIR)

        @pl.loop(0, 2)
        def _(m):
            rows = pl.ds(mul(m * 256, 256), 256)
            part = dot(g_out[rows, cols], wd[cols, :])
            acc_d[rows, :] = part if first else acc_d[rows, :] + part

    def out_step(j):
        cols = pl.ds(mul(j * PAIR, 128), PAIR)

        @pl.loop(0, 2)
        def _(m):
            rows = pl.ds(mul(m * 256, 256), 256)
            eo_out[rows, cols] = dot_nt(hid_out[rows, :], wd[cols, :]).astype(BF16)

    forward_neighbours(2)
    ag_in(2, 2).wait_recv()
    down_step(h, True)
    out_step(h)
    ag_in(2, 5).wait_recv()
    down_step(up_j(3), False)
    out_step(up_j(3))
    ag_in(2, 6).wait_recv()
    down_step(up_j(1), False)
    out_step(up_j(1))
    finish_gather(2)
    wait_opposite(2)
    down_step(up_j(2), False)
    out_step(up_j(2))

    @pl.loop(0, 16)
    def _(m):
        rows = pl.ds(mul(m * 32, 32), 32)
        dh = acc_d[rows, :]
        dg_out[rows, :] = (dh * acc_g[rows, :]).astype(BF16)
        du_out[rows, :] = (dh * acc_u[rows, :]).astype(BF16)

    for cp in zex:
        cp.wait_send()
    for a in range(3):
        for k in range(9):
            ag(a, k).wait_send()
    for bi in range(2):

        @pl.loop(1, 16)
        def _(i):
            for cp in dispatch_copy(bi, i, False):
                cp.wait_send()


def reduce_kernel(
    x, g, hid, dg, du, eo, r_mat, mt,
    gg_out, gu_out, gd_out, mixed_out,
    pd, pg, pu, ra, hs, hr, fs, fr, rets, rr, zsend, zrecv,
    d2s, d2r, hss, hsr, fss, fsr, rs, rr_sem, zs, zr,
):
    me = Place()
    h, c = me.h, me.c
    arrays = ((pd, g, hid), (pg, x, dg), (pu, x, du))
    outs = (gd_out, gg_out, gu_out)

    def up_j(k):
        return (h + k) % 4

    def part_rows(j, core):
        return pl.ds(mul(CHUNK * (2 * j + core), 8), SENT)

    def exchange(a, k):
        return remote(
            arrays[a][0].at[part_rows(up_j(k), 1 - c), :],
            ra.at[a * 4 + k],
            d2s.at[a * 4 + k],
            d2r.at[a * 4 + k],
            me.sibling,
        )

    def half(a, k):
        lo, size = ((0, HALF), (HALF, SENT - HALF))[k]
        return remote(
            hs.at[a, pl.ds(lo, size), :],
            hr.at[a, pl.ds(lo, size), :],
            hss.at[a * 2 + k],
            hsr.at[a * 2 + k],
            (me.up, me.down)[k],
        )

    def full(a, k):
        return remote(
            fs.at[a * 2 + k], fr.at[a * 2 + k], fss.at[a * 2 + k], fsr.at[a * 2 + k], (me.up, me.down)[k]
        )

    def back_copy(bi, i, incoming):
        p, px, py = me.plane(i, -1 if incoming else 1)
        place = p if incoming else me.p
        k = bi * 16 + i
        return remote(
            rets.at[rows_of(me.block(px, py, bi)), :],
            rr.at[pl.ds(mul((bi * 16 + place) * SLOT, 8), SLOT), :],
            rs.at[k],
            rr_sem.at[k],
            me.plane_device(px, py),
        )

    me.greet()

    for a in range(3):
        parts, left, right = arrays[a]
        for k in (2, 1, 3, 0):
            cols = pl.ds(mul(up_j(k) * PAIR, 128), PAIR)
            parts[cols, :] = dot_tn(left[:, cols], right[...]).astype(BF16)
            exchange(a, k).start()
        exchange(a, 2).wait_recv()
        mine = parts[part_rows(up_j(2), c), :]
        hs[a] = (mine.astype(F32) + ra[a * 4 + 2].astype(F32)).astype(BF16)
        half(a, 0).start()
        half(a, 1).start()
        if a == 0:

            @pl.loop(0, 2)
            def _(m):
                cols = pl.ds(mul(m * PLANE, 128), PLANE)
                rets[pl.ds(mul(m * PLANE, 8), PLANE), :] = dot_tn(r_mat[:, cols], eo[...]).astype(BF16)

            for bi in range(2):
                rr[pl.ds(mul((bi * 16 + me.p) * SLOT, 8), SLOT), :] = rets[
                    rows_of(me.block(me.x, me.y, bi)), :
                ]

                @pl.loop(1, 16)
                def _(i):
                    back_copy(bi, i, False).start()

    for a in range(3):
        parts = arrays[a][0]
        for k, jj in ((0, 1), (1, 3)):
            exchange(a, jj).wait_recv()
            half(a, k).wait_recv()
            total = parts[part_rows(up_j(jj), c), :].astype(F32) + ra[a * 4 + jj].astype(F32)
            lo, size = ((0, HALF), (HALF, SENT - HALF))[k]
            fs[a * 2 + k] = total.astype(BF16)
            fs[a * 2 + k, pl.ds(lo, size), :] = (
                total[lo : lo + size] + hr[a, pl.ds(lo, size), :].astype(F32)
            ).astype(BF16)
            full(a, k).start()

    for bi in range(2):

        @pl.loop(1, 16)
        def _(i):
            back_copy(bi, i, True).wait_recv()

    def combine(bi):
        weight = mt[bi]
        high = weight.astype(BF16)
        low = (weight - high.astype(F32)).astype(BF16)
        got = rr[pl.ds(bi * PLANE, PLANE), :]
        return dot_tn(high, got) + dot_tn(low, got)

    zsend[...] = combine(1).astype(BF16)
    zcopy = remote(zsend, zrecv, zs.at[0], zr.at[0], me.partner)
    zcopy.start()
    own = combine(0)
    zcopy.wait_recv()
    mixed_out[...] = (own + zrecv[...].astype(F32)).astype(BF16)

    for a in range(3):
        parts = arrays[a][0]
        exchange(a, 0).wait_recv()
        total = parts[part_rows(h, c), :].astype(F32) + ra[a * 4].astype(F32)
        for k in range(2):
            full(a, k).wait_recv()
            total = total + fr[a * 2 + k].astype(F32)
        outs[a][...] = total.astype(BF16)

    zcopy.wait_send()
    for a in range(3):
        for k in range(4):
            exchange(a, k).wait_send()
        for k in range(2):
            half(a, k).wait_send()
            full(a, k).wait_send()
    for bi in range(2):

        @pl.loop(1, 16)
        def _(i):
            back_copy(bi, i, False).wait_send()


def sds(shape, dtype=BF16):
    return jax.ShapeDtypeStruct(shape, dtype)


def widened(a):
    return jnp.pad(a.reshape(TOK, 8, OWN), ((0, 0), (0, 0), (0, CHUNK - OWN))).reshape(TOK, DP)


def body(tokens, cotangent, expert_ids, gate_weights, w_gate, w_up, w_down):
    lane = lax.broadcasted_iota(jnp.int32, (TOK, DP), 1)
    tok = jnp.where(lane == OWN, jnp.ones((), BF16), widened(tokens))
    cot = widened(cotangent)
    meta = jnp.concatenate([expert_ids.astype(F32), gate_weights], axis=1).T
    shards = [jnp.pad(w[0], ((0, CHUNK - OWN), (0, 0))) for w in (w_gate, w_up, w_down)]
    dma, reg = pltpu.SemaphoreType.DMA, pltpu.SemaphoreType.REGULAR
    mids = pl.pallas_call(
        gather_kernel,
        name="gather",
        out_shape=[
            sds((CAP, DP)), sds((CAP, DP)), sds((CAP, FH)), sds((CAP, FH)), sds((CAP, FH)), sds((CAP, DP)),
            sds((CAP, SLOTS)), sds((2, PLANE, TOK), F32),
        ],
        in_specs=[VM(), VM(), VM()] + [pl.BlockSpec(memory_space=pl.ANY)] * 3,
        out_specs=[VM()] * 8,
        scratch_shapes=[
            pltpu.VMEM((DP, FH), BF16), pltpu.VMEM((DP, FH), BF16), pltpu.VMEM((DP, FH), BF16),
            pltpu.VMEM((8, TOK), F32), pltpu.VMEM((TOK, DP), BF16), pltpu.VMEM((TOK, DP), BF16),
            pltpu.VMEM((SLOTS, DP), BF16), pltpu.VMEM((SLOTS, DP), BF16),
            pltpu.VMEM((SLOTS, DP), BF16), pltpu.VMEM((SLOTS, DP), BF16),
            pltpu.VMEM((CAP, FH), F32), pltpu.VMEM((CAP, FH), F32), pltpu.VMEM((CAP, FH), F32),
            dma((3,)), dma((3,)), dma((3,)), dma((27,)), dma((27,)), dma((64,)), dma((64,)),
        ],
        compiler_params=pltpu.CompilerParams(
            collective_id=0, has_side_effects=True, vmem_limit_bytes=67043328
        ),
    )(meta, tok, cot, *shards)
    gg, gu, gd, mixed = pl.pallas_call(
        reduce_kernel,
        name="reduce",
        out_shape=[sds((SENT, FH)), sds((SENT, FH)), sds((SENT, FH)), sds((TOK, DP))],
        in_specs=[VM()] * 8,
        out_specs=[VM()] * 4,
        scratch_shapes=[
            pltpu.VMEM((DP, FH), BF16), pltpu.VMEM((DP, FH), BF16), pltpu.VMEM((DP, FH), BF16),
            pltpu.VMEM((12, SENT, FH), BF16),
            pltpu.VMEM((3, SENT, FH), BF16), pltpu.VMEM((3, SENT, FH), BF16),
            pltpu.VMEM((6, SENT, FH), BF16), pltpu.VMEM((6, SENT, FH), BF16),
            pltpu.VMEM((SLOTS, DP), BF16), pltpu.VMEM((SLOTS, DP), BF16),
            pltpu.VMEM((TOK, DP), BF16), pltpu.VMEM((TOK, DP), BF16),
            dma((12,)), dma((12,)), dma((6,)), dma((6,)), dma((6,)), dma((6,)),
            dma((32,)), dma((32,)), dma((1,)), dma((1,)),
        ],
        compiler_params=pltpu.CompilerParams(
            collective_id=1, has_side_effects=True, vmem_limit_bytes=67043328
        ),
    )(*mids)
    mixed = mixed.reshape(TOK, 8, CHUNK)[:, :, :OWN].reshape(TOK, D)
    return mixed, gg[None, :OWN], gu[None, :OWN], gd[None, :OWN]


def solution(mesh):
    rows, weight = P(("expert", "dp"), None), P("expert", "dp", None)
    return jax.shard_map(
        body,
        mesh=mesh,
        in_specs=(rows, rows, rows, rows, weight, weight, weight),
        out_specs=(rows, weight, weight, weight),
        check_vma=False,
    )
```

```python
import functools

import jax
import jax.numpy as jnp
from jax import lax
from jax.experimental import pallas as pl
from jax.experimental.pallas import tpu as pltpu
from jax.sharding import PartitionSpec as P

MESH = pl.DeviceIdType.MESH
SWISH_SLOPE = 1.702
F32, BF16 = jnp.float32, jnp.bfloat16
TOK = 128
CAP = 512
SLOT = 24
D = 1440
FH = 1440
OWN = 180
SENT = 184
CHUNK = 192
DP = 8 * CHUNK
PAIR = 2 * CHUNK
HALF = 96
SLOTS = 32 * SLOT
PLANE = 16 * SLOT
VM = functools.partial(pl.BlockSpec, memory_space=pltpu.VMEM)


def mul(value, k):
    return pl.multiple_of(value, k)


class Place:
    def __init__(self):
        e, d = lax.axis_index("expert"), lax.axis_index("dp")
        self.x, self.zl, self.y = e // 8, (e // 4) % 2, e % 4
        self.h, self.c = d // 2, d % 2
        self.e, self.d = e, d
        self.sibling = (e, self.h * 2 + 1 - self.c)
        self.up = (e, ((self.h + 1) % 4) * 2 + self.c)
        self.down = (e, ((self.h + 3) % 4) * 2 + self.c)
        self.partner = (self.x * 8 + (1 - self.zl) * 4 + self.y, d)
        self.p = self.x * 4 + self.y

    def plane(self, i, sign):
        px = (self.x + sign * (i // 4) + 4) % 4
        py = (self.y + sign * (i % 4) + 4) % 4
        return px * 4 + py, px, py

    def plane_device(self, px, py):
        return (px * 8 + self.zl * 4 + py, self.d)

    def block(self, px, py, bi):
        zb = self.zl if bi == 0 else 1 - self.zl
        return px * 8 + zb * 4 + py

    def greet(self):
        barrier = pltpu.get_barrier_semaphore()
        for peer in (self.sibling, self.up, self.down, self.partner):
            pl.semaphore_signal(barrier, inc=1, device_id=peer, device_id_type=MESH)

        @pl.loop(1, 16)
        def _(i):
            _, px, py = self.plane(i, 1)
            pl.semaphore_signal(
                barrier, inc=1, device_id=self.plane_device(px, py), device_id_type=MESH
            )

        pl.semaphore_wait(barrier, 19)


def remote(src, dst, ssem, rsem, device):
    return pltpu.make_async_remote_copy(
        src_ref=src, dst_ref=dst, send_sem=ssem, recv_sem=rsem, device_id=device, device_id_type=MESH
    )


def rows_of(block, size=SLOT):
    return pl.ds(mul(block * SLOT, 8), size)


def dot(a, b):
    return jnp.dot(a, b, preferred_element_type=F32)


def dot_nt(a, b):
    return lax.dot_general(a, b, (((1,), (1,)), ((), ())), preferred_element_type=F32)


def dot_tn(a, b):
    return lax.dot_general(a, b, (((0,), (0,)), ((), ())), preferred_element_type=F32)


def one_zero(flag):
    return jnp.where(flag, 1.0, 0.0)


def step_kernel(
    ids, gates_in, tok_in, cot_in, wg_in, wu_in, wd_in,
    gg_out, gu_out, gd_out, mixed_out,
    wg, wu, wd, meta, zmeta, tok, cot, ztok, zcot, send_x, send_g, recv_x, recv_g,
    x, g, hid, eo, acc_g, acc_u, acc_d, pd, ra_d, hr, fr, rets, rr, r_mat, mt, zsend, zrecv,
    loc_sem, zs, zr, ags, agr, dss, dsr, d2s, d2r, hss, hsr, fss, fsr, rs, rr_sem,
):
    me = Place()
    h, c = me.h, me.c
    weights = (wg, wu, wd)
    outs = (gd_out, gg_out, gu_out)
    dg, du = send_x.at[pl.ds(0, CAP), :], send_g.at[pl.ds(0, CAP), :]

    def up_j(k):
        return (h + k) % 4

    def base(j, core):
        return CHUNK * (2 * j + core)

    def rows_at(j, core, lo=0, size=SENT):
        return pl.ds(mul(base(j, core) + lo, 8), size)

    def shard(w, j, core, lo=0, size=SENT):
        return w.at[rows_at(j, core, lo, size), :]

    staged = (gg_out, gu_out, gd_out)
    own_copies = [
        pltpu.make_async_copy(src.at[0], dst, loc_sem.at[a])
        for a, (src, dst) in enumerate(zip((wg_in, wu_in, wd_in), staged))
    ]
    for cp in own_copies:
        cp.start()
    meta[0:4, :] = ids[...].astype(F32)
    meta[4:8, :] = gates_in[...]
    for ext, src in ((tok, tok_in), (cot, cot_in)):
        for k in range(8):
            ext[CHUNK * k : CHUNK * k + OWN, :] = src[OWN * k : OWN * (k + 1), :]
            live = lax.broadcasted_iota(jnp.int32, (CHUNK - OWN, TOK), 0) == 0
            flag = one_zero(live) if ext is tok and k == 0 else jnp.zeros((CHUNK - OWN, TOK), F32)
            ext[CHUNK * k + OWN : CHUNK * (k + 1), :] = flag.astype(BF16)
    for a, w in enumerate(weights):
        for k in range(8):
            w[pl.ds(CHUNK * k + SENT, CHUNK - SENT), :] = jnp.zeros((CHUNK - SENT, DP), BF16)
        own_copies[a].wait()
        w[rows_at(h, c), FH - 32 :] = jnp.zeros((SENT, DP - FH + 32), BF16)
        w[rows_at(h, c, SENT - 8, 8), :] = jnp.zeros((8, DP), BF16)
        w[rows_at(h, c, 0, OWN), :FH] = staged[a][...]

    me.greet()

    zex = [
        remote(src, dst, zs.at[k], zr.at[k], me.partner)
        for k, (src, dst) in enumerate(((meta, zmeta), (tok, ztok), (cot, zcot)))
    ]
    for cp in zex:
        cp.start()

    def ag(a, k):
        w = weights[a]
        s, r = ags.at[a * 9 + k], agr.at[a * 9 + k]
        if k == 0:
            return remote(shard(w, h, c), shard(w, h, c), s, r, me.up)
        if k == 1:
            return remote(shard(w, h, c), shard(w, h, c), s, r, me.down)
        if k == 2:
            return remote(shard(w, h, c), shard(w, h, c), s, r, me.sibling)
        if k == 3:
            part = shard(w, up_j(3), c, 0, HALF)
            return remote(part, part, s, r, me.up)
        if k == 4:
            part = shard(w, up_j(1), c, HALF, SENT - HALF)
            return remote(part, part, s, r, me.down)
        if k in (5, 6):
            part = shard(w, up_j(3 if k == 5 else 1), c)
            return remote(part, part, s, r, me.sibling)
        part = shard(w, up_j(2), c, 0, HALF) if k == 7 else shard(w, up_j(2), c, HALF, SENT - HALF)
        return remote(part, part, s, r, me.sibling)

    def ag_in(a, k):
        w = weights[a]
        s, r = ags.at[a * 9 + k], agr.at[a * 9 + k]
        lo, size = 0, SENT
        if k == 0:
            j, core = up_j(3), c
        elif k == 1:
            j, core = up_j(1), c
        elif k == 2:
            j, core = h, 1 - c
        elif k == 3:
            j, core, size = up_j(2), c, HALF
        elif k == 4:
            j, core, lo, size = up_j(2), c, HALF, SENT - HALF
        elif k in (5, 6):
            j, core = up_j(3 if k == 5 else 1), 1 - c
        elif k == 7:
            j, core, size = up_j(2), 1 - c, HALF
        else:
            j, core, lo, size = up_j(2), 1 - c, HALF, SENT - HALF
        part = shard(w, j, core, lo, size)
        return remote(part, part, s, r, me.sibling)

    for a in (0, 1):
        for k in (0, 1, 2):
            ag(a, k).start()

    def dispatch_copy(bi, i, incoming):
        p, px, py = me.plane(i, -1 if incoming else 1)
        at = (bi * 16 + p) * SLOT
        source = me.block(px, py, bi) if incoming else me.block(me.x, me.y, bi)
        copies = []
        for arr, (src, dst) in enumerate(((send_x, recv_x), (send_g, recv_g))):
            k = (bi * 2 + arr) * 16 + i
            copies.append(
                remote(
                    src.at[pl.ds(mul(at, 8), SLOT), :],
                    dst.at[rows_of(source), :],
                    dss.at[k],
                    dsr.at[k],
                    me.plane_device(px, py),
                )
            )
        return copies

    def dispatch(bi, m_ref, t_ref, c_ref):
        place = lax.broadcasted_iota(jnp.int32, (16, TOK), 0)
        expert = ((place // 4) * 8 + me.zl * 4 + place % 4).astype(F32)
        named = jnp.zeros((16, TOK), F32)
        gates = jnp.zeros((16, TOK), F32)
        for k in range(4):
            hit = m_ref[k : k + 1, :] == expert
            named = named + one_zero(hit)
            gates = gates + jnp.where(hit, m_ref[4 + k : 5 + k, :], 0.0)
        earlier = one_zero(
            lax.broadcasted_iota(jnp.int32, (TOK, TOK), 0) < lax.broadcasted_iota(jnp.int32, (TOK, TOK), 1)
        ).astype(BF16)
        rank = dot(named.astype(BF16), earlier)
        rank = jnp.where(named > 0.5, rank, -1.0)
        slot = lax.broadcasted_iota(jnp.int32, (16, SLOT, TOK), 1).astype(F32)
        chosen3 = one_zero(slot == rank[:, None, :])
        weighted = (chosen3 * gates[:, None, :]).reshape(PLANE, TOK)
        pick = chosen3.reshape(PLANE, TOK).astype(BF16)
        mt[bi] = weighted
        slot_gate = jnp.sum(weighted, axis=1, keepdims=True)
        send_x[pl.ds(bi * PLANE, PLANE), :] = dot_nt(pick, t_ref[...]).astype(BF16)
        send_g[pl.ds(bi * PLANE, PLANE), :] = (dot_nt(pick, c_ref[...]) * slot_gate).astype(BF16)
        mine = rows_of(me.block(me.x, me.y, bi))
        here = pl.ds(mul((bi * 16 + me.p) * SLOT, 8), SLOT)
        recv_x[mine, :] = send_x[here, :]
        recv_g[mine, :] = send_g[here, :]

        @pl.loop(1, 16)
        def _(i):
            for cp in dispatch_copy(bi, i, False):
                cp.start()

    dispatch(0, meta, tok, cot)
    for cp in zex:
        cp.wait_recv()
    dispatch(1, zmeta, ztok, zcot)

    def forward_neighbours(a):
        ag_in(a, 0).wait_recv()
        ag(a, 3).start()
        ag(a, 5).start()
        ag_in(a, 1).wait_recv()
        ag(a, 4).start()
        ag(a, 6).start()

    forward_neighbours(0)
    forward_neighbours(1)
    for k in (0, 1, 2):
        ag(2, k).start()

    for bi in range(2):

        @pl.loop(1, 16)
        def _(i):
            for cp in dispatch_copy(bi, i, True):
                cp.wait_recv()

    eye_lane = one_zero(lax.broadcasted_iota(jnp.int32, (8, 128), 1) == OWN - 128).astype(BF16)
    flags = dot_nt(eye_lane, recv_x[:, 128:256])
    before = one_zero(
        lax.broadcasted_iota(jnp.int32, (SLOTS, SLOTS), 0) < lax.broadcasted_iota(jnp.int32, (SLOTS, SLOTS), 1)
    ).astype(BF16)
    position = dot(flags.astype(BF16), before)
    position = jnp.where(flags > 0.5, position, -1.0)[0:1, :]

    @pl.loop(0, 2)
    def _(m):
        at = mul(m * 256, 256)
        row = (lax.broadcasted_iota(jnp.int32, (256, SLOTS), 0) + at).astype(F32)
        pick = one_zero(row == position).astype(BF16)
        r_mat[pl.ds(at, 256), :] = pick
        x[pl.ds(at, 256), :] = dot(pick, recv_x[...]).astype(BF16)
        g[pl.ds(at, 256), :] = dot(pick, recv_g[...]).astype(BF16)

    def project(j, first):
        cols = pl.ds(mul(j * PAIR, 128), PAIR)

        @pl.loop(0, 2)
        def _(m):
            rows = pl.ds(mul(m * 256, 256), 256)
            xs = x[rows, cols]
            for acc, w in ((acc_g, wg), (acc_u, wu)):
                part = dot(xs, w[cols, :])
                acc[rows, :] = part if first else acc[rows, :] + part

    for a in (0, 1):
        ag_in(a, 2).wait_recv()
    project(h, True)
    for a in (0, 1):
        ag_in(a, 5).wait_recv()
    project(up_j(3), False)
    for a in (0, 1):
        ag_in(a, 6).wait_recv()
    project(up_j(1), False)

    def finish_gather(a):
        ag_in(a, 3).wait_recv()
        ag(a, 7).start()
        ag_in(a, 4).wait_recv()
        ag(a, 8).start()

    def wait_opposite(a):
        ag_in(a, 7).wait_recv()
        ag_in(a, 8).wait_recv()

    finish_gather(0)
    finish_gather(1)
    wait_opposite(0)
    wait_opposite(1)
    project(up_j(2), False)

    @pl.loop(0, 16)
    def _(m):
        rows = pl.ds(mul(m * 32, 32), 32)
        gate, up = acc_g[rows, :], acc_u[rows, :] + 1.0
        sg = jax.nn.sigmoid(SWISH_SLOPE * gate)
        value = gate * sg
        slope = sg + SWISH_SLOPE * value * (1.0 - sg)
        hid[rows, :] = (value * up).astype(BF16)
        acc_g[rows, :] = up * slope
        acc_u[rows, :] = value

    arrays = ((pd, g, hid), (wg, x, dg), (wu, x, du))

    def ra(a, k):
        if a == 0:
            return ra_d.at[k]
        return (recv_x, recv_g)[a - 1].at[pl.ds(CHUNK * k, SENT), :]

    def exchange(a, k):
        return remote(
            shard(arrays[a][0], up_j(k), 1 - c), ra(a, k), d2s.at[a * 4 + k], d2r.at[a * 4 + k], me.sibling
        )

    def parts_of(a):
        parts, left, right = arrays[a]
        for k in (2, 1, 3, 0):
            cols = pl.ds(mul(up_j(k) * PAIR, 128), PAIR)
            parts[cols, :] = dot_tn(left[:, cols], right[...]).astype(BF16)
            exchange(a, k).start()

    def half(a, k):
        lo, size = ((0, HALF), (HALF, SENT - HALF))[k]
        return remote(
            shard(arrays[a][0], up_j(2), c, lo, size),
            hr.at[a, pl.ds(lo, size), :],
            hss.at[a * 2 + k],
            hsr.at[a * 2 + k],
            (me.up, me.down)[k],
        )

    def full(a, k):
        return remote(
            shard(arrays[a][0], up_j((1, 3)[k]), c),
            fr.at[a * 2 + k],
            fss.at[a * 2 + k],
            fsr.at[a * 2 + k],
            (me.up, me.down)[k],
        )

    def send_halves(a):
        exchange(a, 2).wait_recv()
        rows = rows_at(up_j(2), c)
        parts = arrays[a][0]
        parts[rows, :] = (parts[rows, :].astype(F32) + ra(a, 2)[...].astype(F32)).astype(BF16)
        half(a, 0).start()
        half(a, 1).start()

    def send_fulls(a):
        parts = arrays[a][0]
        for k, jj in ((0, 1), (1, 3)):
            exchange(a, jj).wait_recv()
            half(a, k).wait_recv()
            for with_half in (True, False):
                lo, size = ((0, HALF), (HALF, SENT - HALF))[k if with_half else 1 - k]
                rows = rows_at(up_j(jj), c, lo, size)
                total = parts[rows, :].astype(F32) + ra(a, jj)[lo : lo + size, :].astype(F32)
                if with_half:
                    total = total + hr[a, pl.ds(lo, size), :].astype(F32)
                parts[rows, :] = total.astype(BF16)
            full(a, k).start()

    def down_step(j, first):
        cols = pl.ds(mul(j * PAIR, 128), PAIR)

        @pl.loop(0, 2)
        def _(m):
            rows = pl.ds(mul(m * 256, 256), 256)
            part = dot(g[rows, cols], wd[cols, :])
            acc_d[rows, :] = part if first else acc_d[rows, :] + part

    def out_step(j):
        cols = pl.ds(mul(j * PAIR, 128), PAIR)

        @pl.loop(0, 2)
        def _(m):
            rows = pl.ds(mul(m * 256, 256), 256)
            eo[rows, cols] = dot_nt(hid[rows, :], wd[cols, :]).astype(BF16)

    parts_of(0)
    for cp in zex:
        cp.wait_send()
    for bi in range(2):

        @pl.loop(1, 16)
        def _(i):
            for cp in dispatch_copy(bi, i, False):
                cp.wait_send()

    for a in range(2):
        for k in range(9):
            ag(a, k).wait_send()
    forward_neighbours(2)
    send_halves(0)
    ag_in(2, 2).wait_recv()
    down_step(h, True)
    out_step(h)
    ag_in(2, 5).wait_recv()
    down_step(up_j(3), False)
    ag_in(2, 6).wait_recv()
    down_step(up_j(1), False)
    finish_gather(2)
    wait_opposite(2)
    down_step(up_j(2), False)

    @pl.loop(0, 16)
    def _(m):
        rows = pl.ds(mul(m * 32, 32), 32)
        dh = acc_d[rows, :]
        dg[rows, :] = (dh * acc_g[rows, :]).astype(BF16)
        du[rows, :] = (dh * acc_u[rows, :]).astype(BF16)

    parts_of(1)
    send_halves(1)
    send_fulls(0)
    parts_of(2)
    send_halves(2)
    for k in (3, 1, 2):
        out_step(up_j(k))

    def back_copy(bi, i, incoming):
        p, px, py = me.plane(i, -1 if incoming else 1)
        place = p if incoming else me.p
        k = bi * 16 + i
        return remote(
            rets.at[rows_of(me.block(px, py, bi)), :],
            rr.at[pl.ds(mul((bi * 16 + place) * SLOT, 8), SLOT), :],
            rs.at[k],
            rr_sem.at[k],
            me.plane_device(px, py),
        )

    @pl.loop(0, 2)
    def _(m):
        cols = pl.ds(mul(m * PLANE, 128), PLANE)
        rets[pl.ds(mul(m * PLANE, 8), PLANE), :] = dot_tn(r_mat[:, cols], eo[...]).astype(BF16)

    for bi in range(2):
        rr[pl.ds(mul((bi * 16 + me.p) * SLOT, 8), SLOT), :] = rets[rows_of(me.block(me.x, me.y, bi)), :]

        @pl.loop(1, 16)
        def _(i):
            back_copy(bi, i, False).start()

    send_fulls(1)

    for bi in range(2):

        @pl.loop(1, 16)
        def _(i):
            back_copy(bi, i, True).wait_recv()

    def combine(bi):
        weight = mt[bi]
        high = weight.astype(BF16)
        low = (weight - high.astype(F32)).astype(BF16)
        both = dot_tn(rr[pl.ds(bi * PLANE, PLANE), :], jnp.concatenate([high, low], axis=1))
        return both[:, :TOK] + both[:, TOK:]

    zsend[...] = combine(1).astype(BF16)
    zcopy = remote(zsend, zrecv, zs.at[3], zr.at[3], me.partner)
    zcopy.start()
    send_fulls(2)
    own = combine(0)
    zcopy.wait_recv()
    mixed = (own + zrecv[...].astype(F32)).astype(BF16)
    for k in range(8):
        mixed_out[OWN * k : OWN * (k + 1), :] = mixed[CHUNK * k : CHUNK * k + OWN, :]

    for a in range(3):
        exchange(a, 0).wait_recv()
        total = arrays[a][0][rows_at(h, c), :].astype(F32) + ra(a, 0)[...].astype(F32)
        for k in range(2):
            full(a, k).wait_recv()
            total = total + fr[a * 2 + k].astype(F32)
        outs[a][...] = total.astype(BF16)[:OWN, :FH]

    zcopy.wait_send()
    for k in range(9):
        ag(2, k).wait_send()
    for a in range(3):
        for k in range(4):
            exchange(a, k).wait_send()
        for k in range(2):
            half(a, k).wait_send()
            full(a, k).wait_send()
    for bi in range(2):

        @pl.loop(1, 16)
        def _(i):
            back_copy(bi, i, False).wait_send()


def body(tokens, cotangent, expert_ids, gate_weights, w_gate, w_up, w_down):
    dma = pltpu.SemaphoreType.DMA
    b16 = lambda *shape: pltpu.VMEM(shape, BF16)
    f32 = lambda *shape: pltpu.VMEM(shape, F32)
    gg, gu, gd, mixed = pl.pallas_call(
        step_kernel,
        name="step",
        out_shape=[jax.ShapeDtypeStruct((OWN, FH), BF16)] * 3 + [jax.ShapeDtypeStruct((D, TOK), BF16)],
        in_specs=[VM()] * 4 + [pl.BlockSpec(memory_space=pl.ANY)] * 3,
        out_specs=[VM()] * 4,
        scratch_shapes=[
            b16(DP, DP), b16(DP, DP), b16(DP, DP),
            f32(8, TOK), f32(8, TOK), b16(DP, TOK), b16(DP, TOK), b16(DP, TOK), b16(DP, TOK),
            b16(SLOTS, DP), b16(SLOTS, DP), b16(SLOTS, DP), b16(SLOTS, DP),
            b16(CAP, DP), b16(CAP, DP), b16(CAP, DP), b16(CAP, DP),
            f32(CAP, DP), f32(CAP, DP), f32(CAP, DP),
            b16(DP, DP), b16(4, SENT, DP), b16(3, SENT, DP), b16(6, SENT, DP),
            b16(SLOTS, DP), b16(SLOTS, DP), b16(CAP, SLOTS), f32(2, PLANE, TOK), b16(DP, TOK), b16(DP, TOK),
            dma((3,)), dma((4,)), dma((4,)), dma((27,)), dma((27,)), dma((64,)), dma((64,)),
            dma((12,)), dma((12,)), dma((6,)), dma((6,)), dma((6,)), dma((6,)), dma((32,)), dma((32,)),
        ],
        compiler_params=pltpu.CompilerParams(
            collective_id=0, has_side_effects=True, vmem_limit_bytes=67043328
        ),
    )(expert_ids.T, gate_weights.T, tokens.T, cotangent.T, w_gate, w_up, w_down)
    return mixed.T, gg[None], gu[None], gd[None]


def solution(mesh):
    rows, weight = P(("expert", "dp"), None), P("expert", "dp", None)
    return jax.shard_map(
        body,
        mesh=mesh,
        in_specs=(rows, rows, rows, rows, weight, weight, weight),
        out_specs=(rows, weight, weight, weight),
        check_vma=False,
    )
```

```python
import functools

import jax
import jax.numpy as jnp
from jax import lax
from jax.experimental import pallas as pl
from jax.experimental.pallas import tpu as pltpu
from jax.sharding import PartitionSpec as P

MESH = pl.DeviceIdType.MESH
SWISH_SLOPE = 1.702
F32, BF16 = jnp.float32, jnp.bfloat16
TOK = 128
CAP = 512
SLOT = 24
D = 1440
FH = 1440
OWN = 180
SENT = 184
CHUNK = 192
DP = 8 * CHUNK
PAIR = 2 * CHUNK
MAIN = 1408
REST = FH - MAIN
HALF = 96
SLOTS = 32 * SLOT
PLANE = 16 * SLOT
VM = functools.partial(pl.BlockSpec, memory_space=pltpu.VMEM)


def mul(value, k):
    return pl.multiple_of(value, k)


class Place:
    def __init__(self):
        e, d = lax.axis_index("expert"), lax.axis_index("dp")
        self.x, self.zl, self.y = e // 8, (e // 4) % 2, e % 4
        self.h, self.c = d // 2, d % 2
        self.e, self.d = e, d
        self.sibling = (e, self.h * 2 + 1 - self.c)
        self.up = (e, ((self.h + 1) % 4) * 2 + self.c)
        self.down = (e, ((self.h + 3) % 4) * 2 + self.c)
        self.partner = (self.x * 8 + (1 - self.zl) * 4 + self.y, d)
        self.p = self.x * 4 + self.y

    def plane(self, i, sign):
        px = (self.x + sign * (i // 4) + 4) % 4
        py = (self.y + sign * (i % 4) + 4) % 4
        return px * 4 + py, px, py

    def plane_device(self, px, py):
        return (px * 8 + self.zl * 4 + py, self.d)

    def block(self, px, py, bi):
        zb = self.zl if bi == 0 else 1 - self.zl
        return px * 8 + zb * 4 + py

    def greet(self):
        barrier = pltpu.get_barrier_semaphore()
        for peer in (self.sibling, self.up, self.down, self.partner):
            pl.semaphore_signal(barrier, inc=1, device_id=peer, device_id_type=MESH)

        @pl.loop(1, 16)
        def _(i):
            _, px, py = self.plane(i, 1)
            pl.semaphore_signal(
                barrier, inc=1, device_id=self.plane_device(px, py), device_id_type=MESH
            )

        pl.semaphore_wait(barrier, 19)


def remote(src, dst, ssem, rsem, device):
    return pltpu.make_async_remote_copy(
        src_ref=src, dst_ref=dst, send_sem=ssem, recv_sem=rsem, device_id=device, device_id_type=MESH
    )


def rows_of(block, size=SLOT):
    return pl.ds(mul(block * SLOT, 8), size)


def dot(a, b):
    return jnp.dot(a, b, preferred_element_type=F32)


def dot_nt(a, b):
    return lax.dot_general(a, b, (((1,), (1,)), ((), ())), preferred_element_type=F32)


def dot_tn(a, b):
    return lax.dot_general(a, b, (((0,), (0,)), ((), ())), preferred_element_type=F32)


def one_zero(flag):
    return jnp.where(flag, 1.0, 0.0)


def step_kernel(
    ids, gates_in, tok_in, cot_in, wg_in, wu_in, wd_in,
    gg_out, gu_out, gd_out, mixed_out,
    wg, wu, wd, wrem, grem, ra_rem, hr_rem, fr_rem, meta, zmeta, tok, cot, ztok, zcot, send_x, send_g, recv_x, recv_g,
    x, g, hid, eo, acc_g, acc_u, acc_d, pd, ra_d, hr, fr, rets, rr, r_mat, mt, zsend, zrecv,
    loc_sem, zs, zr, ags, agr, dss, dsr, d2s, d2r, hss, hsr, fss, fsr, rs, rr_sem,
):
    me = Place()
    h, c = me.h, me.c
    weights = (wg, wu, wd, wrem)
    outs = (gd_out, gg_out, gu_out)
    dg, du = send_x.at[pl.ds(0, CAP), :], send_g.at[pl.ds(0, CAP), :]

    def up_j(k):
        return (h + k) % 4

    def base(j, core):
        return CHUNK * (2 * j + core)

    def rows_at(j, core, lo=0, size=SENT):
        return pl.ds(mul(base(j, core) + lo, 8), size)

    def width(a):
        return pl.ds(0, MAIN if a < 3 else 128)

    def shard(a, w, j, core, lo=0, size=SENT):
        return w.at[rows_at(j, core, lo, size), width(a)]

    staged = (gg_out, gu_out, gd_out)
    own_copies = [
        pltpu.make_async_copy(src.at[0], dst, loc_sem.at[a])
        for a, (src, dst) in enumerate(zip((wg_in, wu_in, wd_in), staged))
    ]
    for cp in own_copies:
        cp.start()
    meta[0:4, :] = ids[...].astype(F32)
    meta[4:8, :] = gates_in[...]
    for ext, src in ((tok, tok_in), (cot, cot_in)):
        for k in range(8):
            ext[CHUNK * k : CHUNK * k + OWN, :] = src[OWN * k : OWN * (k + 1), :]
            live = lax.broadcasted_iota(jnp.int32, (CHUNK - OWN, TOK), 0) == 0
            flag = one_zero(live) if ext is tok and k == 0 else jnp.zeros((CHUNK - OWN, TOK), F32)
            ext[CHUNK * k + OWN : CHUNK * (k + 1), :] = flag.astype(BF16)
    for a, w in enumerate(weights):
        lanes = w.shape[1]
        for k in range(8):
            w[pl.ds(CHUNK * k + SENT, CHUNK - SENT), :] = jnp.zeros((CHUNK - SENT, lanes), BF16)
        w[rows_at(h, c, SENT - 8, 8), :] = jnp.zeros((8, lanes), BF16)
        if a < 3:
            own_copies[a].wait()
            w[rows_at(h, c, 0, OWN), :MAIN] = staged[a][:, :MAIN]
    wrem[rows_at(h, c, 0, OWN), :] = jnp.concatenate(
        [ref[:, MAIN:] for ref in staged] + [jnp.zeros((OWN, 128 - 3 * REST), BF16)], axis=1
    )

    me.greet()

    zex = [
        remote(src, dst, zs.at[k], zr.at[k], me.partner)
        for k, (src, dst) in enumerate(((meta, zmeta), (tok, ztok), (cot, zcot)))
    ]
    for cp in zex:
        cp.start()

    def ag(a, k):
        w = weights[a]
        s, r = ags.at[a * 9 + k], agr.at[a * 9 + k]
        if k == 0:
            return remote(shard(a, w, h, c), shard(a, w, h, c), s, r, me.up)
        if k == 1:
            return remote(shard(a, w, h, c), shard(a, w, h, c), s, r, me.down)
        if k == 2:
            return remote(shard(a, w, h, c), shard(a, w, h, c), s, r, me.sibling)
        if k == 3:
            part = shard(a, w, up_j(3), c, 0, HALF)
            return remote(part, part, s, r, me.up)
        if k == 4:
            part = shard(a, w, up_j(1), c, HALF, SENT - HALF)
            return remote(part, part, s, r, me.down)
        if k in (5, 6):
            part = shard(a, w, up_j(3 if k == 5 else 1), c)
            return remote(part, part, s, r, me.sibling)
        part = shard(a, w, up_j(2), c, 0, HALF) if k == 7 else shard(a, w, up_j(2), c, HALF, SENT - HALF)
        return remote(part, part, s, r, me.sibling)

    def ag_in(a, k):
        w = weights[a]
        s, r = ags.at[a * 9 + k], agr.at[a * 9 + k]
        lo, size = 0, SENT
        if k == 0:
            j, core = up_j(3), c
        elif k == 1:
            j, core = up_j(1), c
        elif k == 2:
            j, core = h, 1 - c
        elif k == 3:
            j, core, size = up_j(2), c, HALF
        elif k == 4:
            j, core, lo, size = up_j(2), c, HALF, SENT - HALF
        elif k in (5, 6):
            j, core = up_j(3 if k == 5 else 1), 1 - c
        elif k == 7:
            j, core, size = up_j(2), 1 - c, HALF
        else:
            j, core, lo, size = up_j(2), 1 - c, HALF, SENT - HALF
        part = shard(a, w, j, core, lo, size)
        return remote(part, part, s, r, me.sibling)

    for a in (3, 0, 1):
        for k in (0, 1, 2):
            ag(a, k).start()

    def dispatch_copy(bi, i, incoming):
        p, px, py = me.plane(i, -1 if incoming else 1)
        at = (bi * 16 + p) * SLOT
        source = me.block(px, py, bi) if incoming else me.block(me.x, me.y, bi)
        copies = []
        for arr, (src, dst) in enumerate(((send_x, recv_x), (send_g, recv_g))):
            k = (bi * 2 + arr) * 16 + i
            copies.append(
                remote(
                    src.at[pl.ds(mul(at, 8), SLOT), :],
                    dst.at[rows_of(source), :],
                    dss.at[k],
                    dsr.at[k],
                    me.plane_device(px, py),
                )
            )
        return copies

    def dispatch(bi, m_ref, t_ref, c_ref):
        place = lax.broadcasted_iota(jnp.int32, (16, TOK), 0)
        expert = ((place // 4) * 8 + me.zl * 4 + place % 4).astype(F32)
        named = jnp.zeros((16, TOK), F32)
        gates = jnp.zeros((16, TOK), F32)
        for k in range(4):
            hit = m_ref[k : k + 1, :] == expert
            named = named + one_zero(hit)
            gates = gates + jnp.where(hit, m_ref[4 + k : 5 + k, :], 0.0)
        earlier = one_zero(
            lax.broadcasted_iota(jnp.int32, (TOK, TOK), 0) < lax.broadcasted_iota(jnp.int32, (TOK, TOK), 1)
        ).astype(BF16)
        rank = dot(named.astype(BF16), earlier)
        rank = jnp.where(named > 0.5, rank, -1.0)
        slot = lax.broadcasted_iota(jnp.int32, (16, SLOT, TOK), 1).astype(F32)
        chosen3 = one_zero(slot == rank[:, None, :])
        weighted = (chosen3 * gates[:, None, :]).reshape(PLANE, TOK)
        pick = chosen3.reshape(PLANE, TOK).astype(BF16)
        mt[bi] = weighted
        slot_gate = jnp.sum(weighted, axis=1, keepdims=True)
        send_x[pl.ds(bi * PLANE, PLANE), :] = dot_nt(pick, t_ref[...]).astype(BF16)
        send_g[pl.ds(bi * PLANE, PLANE), :] = (dot_nt(pick, c_ref[...]) * slot_gate).astype(BF16)
        mine = rows_of(me.block(me.x, me.y, bi))
        here = pl.ds(mul((bi * 16 + me.p) * SLOT, 8), SLOT)
        recv_x[mine, :] = send_x[here, :]
        recv_g[mine, :] = send_g[here, :]

        @pl.loop(1, 16)
        def _(i):
            for cp in dispatch_copy(bi, i, False):
                cp.start()

    dispatch(0, meta, tok, cot)
    for cp in zex:
        cp.wait_recv()
    dispatch(1, zmeta, ztok, zcot)

    def forward_neighbours(a):
        ag_in(a, 0).wait_recv()
        ag(a, 3).start()
        ag(a, 5).start()
        ag_in(a, 1).wait_recv()
        ag(a, 4).start()
        ag(a, 6).start()

    forward_neighbours(3)
    forward_neighbours(0)
    forward_neighbours(1)
    for k in (0, 1, 2):
        ag(2, k).start()

    for bi in range(2):

        @pl.loop(1, 16)
        def _(i):
            for cp in dispatch_copy(bi, i, True):
                cp.wait_recv()

    eye_lane = one_zero(lax.broadcasted_iota(jnp.int32, (8, 128), 1) == OWN - 128).astype(BF16)
    flags = dot_nt(eye_lane, recv_x[:, 128:256])
    before = one_zero(
        lax.broadcasted_iota(jnp.int32, (SLOTS, SLOTS), 0) < lax.broadcasted_iota(jnp.int32, (SLOTS, SLOTS), 1)
    ).astype(BF16)
    position = dot(flags.astype(BF16), before)
    position = jnp.where(flags > 0.5, position, -1.0)[0:1, :]

    @pl.loop(0, 2)
    def _(m):
        at = mul(m * 256, 256)
        row = (lax.broadcasted_iota(jnp.int32, (256, SLOTS), 0) + at).astype(F32)
        pick = one_zero(row == position).astype(BF16)
        r_mat[pl.ds(at, 256), :] = pick
        x[pl.ds(at, 256), :] = dot(pick, recv_x[...]).astype(BF16)
        g[pl.ds(at, 256), :] = dot(pick, recv_g[...]).astype(BF16)

    def project(j, first):
        cols = pl.ds(mul(j * PAIR, 128), PAIR)
        rest = wrem[cols, :].astype(F32)
        lane = lax.broadcasted_iota(jnp.int32, (PAIR, 128), 1)
        for a in range(3):
            own = rest if a == 0 else pltpu.roll(rest, 128 - REST * a, 1)
            weights[a][cols, MAIN:] = jnp.where(lane < REST, own, 0.0).astype(BF16)

        @pl.loop(0, 2)
        def _(m):
            rows = pl.ds(mul(m * 256, 256), 256)
            xs = x[rows, cols]
            for acc, w in ((acc_g, wg), (acc_u, wu)):
                part = dot(xs, w[cols, :])
                acc[rows, :] = part if first else acc[rows, :] + part

    for a in (3, 0, 1):
        ag_in(a, 2).wait_recv()
    project(h, True)
    for a in (3, 0, 1):
        ag_in(a, 5).wait_recv()
    project(up_j(3), False)
    for a in (3, 0, 1):
        ag_in(a, 6).wait_recv()
    project(up_j(1), False)

    def finish_gather(a):
        ag_in(a, 3).wait_recv()
        ag(a, 7).start()
        ag_in(a, 4).wait_recv()
        ag(a, 8).start()

    def wait_opposite(a):
        ag_in(a, 7).wait_recv()
        ag_in(a, 8).wait_recv()

    for a in (3, 0, 1):
        finish_gather(a)
    for a in (3, 0, 1):
        wait_opposite(a)
    project(up_j(2), False)

    @pl.loop(0, 16)
    def _(m):
        rows = pl.ds(mul(m * 32, 32), 32)
        gate, up = acc_g[rows, :], acc_u[rows, :] + 1.0
        sg = jax.nn.sigmoid(SWISH_SLOPE * gate)
        value = gate * sg
        slope = sg + SWISH_SLOPE * value * (1.0 - sg)
        hid[rows, :] = (value * up).astype(BF16)
        acc_g[rows, :] = up * slope
        acc_u[rows, :] = value

    arrays = ((pd, g, hid), (wg, x, dg), (wu, x, du), (grem, None, None))

    def ra(a, k):
        if a in (0, 3):
            return (ra_d if a == 0 else ra_rem).at[k]
        return (recv_x, recv_g)[a - 1].at[pl.ds(CHUNK * k, SENT), width(a)]

    def half_in(a, lo, size):
        return hr.at[a, pl.ds(lo, size), :] if a < 3 else hr_rem.at[pl.ds(lo, size), :]

    def full_in(a, k):
        return fr.at[a * 2 + k] if a < 3 else fr_rem.at[k]

    def exchange(a, k):
        return remote(
            shard(a, arrays[a][0], up_j(k), 1 - c), ra(a, k), d2s.at[a * 4 + k], d2r.at[a * 4 + k], me.sibling
        )

    def parts_of(a, ks):
        parts, left, right = arrays[a]
        for k in ks:
            cols = pl.ds(mul(up_j(k) * PAIR, 128), PAIR)
            part = dot_tn(left[:, cols], right[...])
            parts[cols, :MAIN] = part[:, :MAIN].astype(BF16)
            exchange(a, k).start()
            rest = part[:, MAIN:]
            if a > 0:
                rest = grem[cols, :].astype(F32) + pltpu.roll(rest, REST * a, 1)
            grem[cols, :] = rest.astype(BF16)
            if a == 2:
                exchange(3, k).start()

    def half(a, k):
        lo, size = ((0, HALF), (HALF, SENT - HALF))[k]
        return remote(
            shard(a, arrays[a][0], up_j(2), c, lo, size),
            half_in(a, lo, size),
            hss.at[a * 2 + k],
            hsr.at[a * 2 + k],
            (me.up, me.down)[k],
        )

    def full(a, k):
        return remote(
            shard(a, arrays[a][0], up_j((1, 3)[k]), c),
            full_in(a, k),
            fss.at[a * 2 + k],
            fsr.at[a * 2 + k],
            (me.up, me.down)[k],
        )

    def send_halves(a):
        exchange(a, 2).wait_recv()
        at = rows_at(up_j(2), c), width(a)
        parts = arrays[a][0]
        parts[at] = (parts[at].astype(F32) + ra(a, 2)[...].astype(F32)).astype(BF16)
        half(a, 0).start()
        half(a, 1).start()

    def send_fulls(a):
        parts = arrays[a][0]
        for k, jj in ((0, 1), (1, 3)):
            exchange(a, jj).wait_recv()
            half(a, k).wait_recv()
            for with_half in (True, False):
                lo, size = ((0, HALF), (HALF, SENT - HALF))[k if with_half else 1 - k]
                at = rows_at(up_j(jj), c, lo, size), width(a)
                total = parts[at].astype(F32) + ra(a, jj)[lo : lo + size, :].astype(F32)
                if with_half:
                    total = total + half_in(a, lo, size)[...].astype(F32)
                parts[at] = total.astype(BF16)
            full(a, k).start()

    def down_step(j, first):
        cols = pl.ds(mul(j * PAIR, 128), PAIR)

        @pl.loop(0, 2)
        def _(m):
            rows = pl.ds(mul(m * 256, 256), 256)
            part = dot(g[rows, cols], wd[cols, :])
            acc_d[rows, :] = part if first else acc_d[rows, :] + part

    def out_step(j):
        cols = pl.ds(mul(j * PAIR, 128), PAIR)

        @pl.loop(0, 2)
        def _(m):
            rows = pl.ds(mul(m * 256, 256), 256)
            eo[rows, cols] = dot_nt(hid[rows, :], wd[cols, :]).astype(BF16)

    parts_of(0, (2, 1, 3, 0))
    for cp in zex:
        cp.wait_send()
    for bi in range(2):

        @pl.loop(1, 16)
        def _(i):
            for cp in dispatch_copy(bi, i, False):
                cp.wait_send()

    for a in (3, 0, 1):
        for k in range(9):
            ag(a, k).wait_send()
    forward_neighbours(2)
    send_halves(0)
    ag_in(2, 2).wait_recv()
    down_step(h, True)
    out_step(h)
    ag_in(2, 5).wait_recv()
    down_step(up_j(3), False)
    ag_in(2, 6).wait_recv()
    down_step(up_j(1), False)
    finish_gather(2)
    wait_opposite(2)
    down_step(up_j(2), False)

    @pl.loop(0, 16)
    def _(m):
        rows = pl.ds(mul(m * 32, 32), 32)
        dh = acc_d[rows, :]
        dg[rows, :] = (dh * acc_g[rows, :]).astype(BF16)
        du[rows, :] = (dh * acc_u[rows, :]).astype(BF16)

    parts_of(1, (2, 1))
    send_halves(1)
    send_fulls(0)
    parts_of(1, (3, 0))
    parts_of(2, (2, 1))
    send_halves(2)
    send_halves(3)
    parts_of(2, (3, 0))
    for k in (3, 1, 2):
        out_step(up_j(k))

    def back_copy(bi, i, incoming):
        p, px, py = me.plane(i, -1 if incoming else 1)
        place = p if incoming else me.p
        k = bi * 16 + i
        return remote(
            rets.at[rows_of(me.block(px, py, bi)), :],
            rr.at[pl.ds(mul((bi * 16 + place) * SLOT, 8), SLOT), :],
            rs.at[k],
            rr_sem.at[k],
            me.plane_device(px, py),
        )

    @pl.loop(0, 2)
    def _(m):
        cols = pl.ds(mul(m * PLANE, 128), PLANE)
        rets[pl.ds(mul(m * PLANE, 8), PLANE), :] = dot_tn(r_mat[:, cols], eo[...]).astype(BF16)

    for bi in range(2):
        rr[pl.ds(mul((bi * 16 + me.p) * SLOT, 8), SLOT), :] = rets[rows_of(me.block(me.x, me.y, bi)), :]

        @pl.loop(1, 16)
        def _(i):
            back_copy(bi, i, False).start()

    send_fulls(1)

    for bi in range(2):

        @pl.loop(1, 16)
        def _(i):
            back_copy(bi, i, True).wait_recv()

    def combine(bi):
        weight = mt[bi]
        high = weight.astype(BF16)
        low = (weight - high.astype(F32)).astype(BF16)
        both = dot_tn(rr[pl.ds(bi * PLANE, PLANE), :], jnp.concatenate([high, low], axis=1))
        return both[:, :TOK] + both[:, TOK:]

    zsend[...] = combine(1).astype(BF16)
    zcopy = remote(zsend, zrecv, zs.at[3], zr.at[3], me.partner)
    zcopy.start()
    send_fulls(2)
    send_fulls(3)
    own = combine(0)
    zcopy.wait_recv()
    mixed = (own + zrecv[...].astype(F32)).astype(BF16)
    for k in range(8):
        mixed_out[OWN * k : OWN * (k + 1), :] = mixed[CHUNK * k : CHUNK * k + OWN, :]

    for a in range(4):
        exchange(a, 0).wait_recv()
        total = arrays[a][0][rows_at(h, c), width(a)].astype(F32) + ra(a, 0)[...].astype(F32)
        for k in range(2):
            full(a, k).wait_recv()
            total = total + full_in(a, k)[...].astype(F32)
        if a < 3:
            outs[a][:, :MAIN] = total.astype(BF16)[:OWN]
        else:
            for b in range(3):
                own = total if b == 0 else pltpu.roll(total, 128 - REST * b, 1)
                outs[b][:, MAIN:] = own.astype(BF16)[:OWN, :REST]

    zcopy.wait_send()
    for k in range(9):
        ag(2, k).wait_send()
    for a in range(4):
        for k in range(4):
            exchange(a, k).wait_send()
        for k in range(2):
            half(a, k).wait_send()
            full(a, k).wait_send()
    for bi in range(2):

        @pl.loop(1, 16)
        def _(i):
            back_copy(bi, i, False).wait_send()


def body(tokens, cotangent, expert_ids, gate_weights, w_gate, w_up, w_down):
    dma = pltpu.SemaphoreType.DMA
    b16 = lambda *shape: pltpu.VMEM(shape, BF16)
    f32 = lambda *shape: pltpu.VMEM(shape, F32)
    gg, gu, gd, mixed = pl.pallas_call(
        step_kernel,
        name="step",
        out_shape=[jax.ShapeDtypeStruct((OWN, FH), BF16)] * 3 + [jax.ShapeDtypeStruct((D, TOK), BF16)],
        in_specs=[VM()] * 4 + [pl.BlockSpec(memory_space=pl.ANY)] * 3,
        out_specs=[VM()] * 4,
        scratch_shapes=[
            b16(DP, DP), b16(DP, DP), b16(DP, DP), b16(DP, 128), b16(DP, 128),
            b16(4, SENT, 128), b16(SENT, 128), b16(2, SENT, 128),
            f32(8, TOK), f32(8, TOK), b16(DP, TOK), b16(DP, TOK), b16(DP, TOK), b16(DP, TOK),
            b16(SLOTS, DP), b16(SLOTS, DP), b16(SLOTS, DP), b16(SLOTS, DP),
            b16(CAP, DP), b16(CAP, DP), b16(CAP, DP), b16(CAP, DP),
            f32(CAP, DP), f32(CAP, DP), f32(CAP, DP),
            b16(DP, DP), b16(4, SENT, MAIN), b16(3, SENT, MAIN), b16(6, SENT, MAIN),
            b16(SLOTS, DP), b16(SLOTS, DP), b16(CAP, SLOTS), f32(2, PLANE, TOK), b16(DP, TOK), b16(DP, TOK),
            dma((3,)), dma((4,)), dma((4,)), dma((36,)), dma((36,)), dma((64,)), dma((64,)),
            dma((16,)), dma((16,)), dma((8,)), dma((8,)), dma((8,)), dma((8,)), dma((32,)), dma((32,)),
        ],
        compiler_params=pltpu.CompilerParams(
            collective_id=0, has_side_effects=True, vmem_limit_bytes=67043328
        ),
    )(expert_ids.T, gate_weights.T, tokens.T, cotangent.T, w_gate, w_up, w_down)
    return mixed.T, gg[None], gu[None], gd[None]


def solution(mesh):
    rows, weight = P(("expert", "dp"), None), P("expert", "dp", None)
    return jax.shard_map(
        body,
        mesh=mesh,
        in_specs=(rows, rows, rows, rows, weight, weight, weight),
        out_specs=(rows, weight, weight, weight),
        check_vma=False,
    )
```

```python
import functools

import jax
import jax.numpy as jnp
from jax import lax
from jax.experimental import pallas as pl
from jax.experimental.pallas import tpu as pltpu
from jax.sharding import PartitionSpec as P

MESH = pl.DeviceIdType.MESH
SWISH_SLOPE = 1.702
F32, BF16 = jnp.float32, jnp.bfloat16
TOK = 128
CAP = 512
SLOT = 24
D = 1440
FH = 1440
OWN = 180
SENT = 184
CHUNK = 192
DP = 8 * CHUNK
PAIR = 2 * CHUNK
MAIN = 1408
REST = FH - MAIN
HALF = 96
SLOTS = 32 * SLOT
PLANE = 16 * SLOT
VM = functools.partial(pl.BlockSpec, memory_space=pltpu.VMEM)


def mul(value, k):
    return pl.multiple_of(value, k)


class Place:
    def __init__(self):
        e, d = lax.axis_index("expert"), lax.axis_index("dp")
        self.x, self.zl, self.y = e // 8, (e // 4) % 2, e % 4
        self.h, self.c = d // 2, d % 2
        self.e, self.d = e, d
        self.sibling = (e, self.h * 2 + 1 - self.c)
        self.up = (e, ((self.h + 1) % 4) * 2 + self.c)
        self.down = (e, ((self.h + 3) % 4) * 2 + self.c)
        self.partner = (self.x * 8 + (1 - self.zl) * 4 + self.y, d)
        self.p = self.x * 4 + self.y

    def plane(self, i, sign):
        px = (self.x + sign * (i // 4) + 4) % 4
        py = (self.y + sign * (i % 4) + 4) % 4
        return px * 4 + py, px, py

    def plane_device(self, px, py):
        return (px * 8 + self.zl * 4 + py, self.d)

    def block(self, px, py, bi):
        zb = self.zl if bi == 0 else 1 - self.zl
        return px * 8 + zb * 4 + py

    def greet(self):
        barrier = pltpu.get_barrier_semaphore()
        for peer in (self.sibling, self.up, self.down, self.partner):
            pl.semaphore_signal(barrier, inc=1, device_id=peer, device_id_type=MESH)

        @pl.loop(1, 16)
        def _(i):
            _, px, py = self.plane(i, 1)
            pl.semaphore_signal(
                barrier, inc=1, device_id=self.plane_device(px, py), device_id_type=MESH
            )

    def await_greetings(self):
        pl.semaphore_wait(pltpu.get_barrier_semaphore(), 19)


def remote(src, dst, ssem, rsem, device):
    return pltpu.make_async_remote_copy(
        src_ref=src, dst_ref=dst, send_sem=ssem, recv_sem=rsem, device_id=device, device_id_type=MESH
    )


def rows_of(block, size=SLOT):
    return pl.ds(mul(block * SLOT, 8), size)


def dot(a, b):
    return jnp.dot(a, b, preferred_element_type=F32)


def dot_nt(a, b):
    return lax.dot_general(a, b, (((1,), (1,)), ((), ())), preferred_element_type=F32)


def dot_tn(a, b):
    return lax.dot_general(a, b, (((0,), (0,)), ((), ())), preferred_element_type=F32)


def one_zero(flag):
    return jnp.where(flag, 1.0, 0.0)


def step_kernel(
    ids, gates_in, tok_in, cot_in, wg_in, wu_in, wd_in,
    gg_out, gu_out, gd_out, mixed_out,
    wg, wu, wd, wrem, grem, ra_rem, hr_rem, fr_rem, meta, zmeta, tok, cot, ztok, zcot, send_x, send_g, recv_x, recv_g,
    x, g, hid, eo, acc_g, acc_u, acc_d, pd, ra_d, hr, fr, rets, rr, r_mat, mt, zsend, zrecv,
    loc_sem, zs, zr, ags, agr, dss, dsr, d2s, d2r, hss, hsr, fss, fsr, rs, rr_sem,
):
    me = Place()
    me.greet()
    h, c = me.h, me.c
    weights = (wg, wu, wd, wrem)
    outs = (gd_out, gg_out, gu_out)
    dg, du = send_x.at[pl.ds(0, CAP), :], send_g.at[pl.ds(0, CAP), :]

    def up_j(k):
        return (h + k) % 4

    def base(j, core):
        return CHUNK * (2 * j + core)

    def rows_at(j, core, lo=0, size=SENT):
        return pl.ds(mul(base(j, core) + lo, 8), size)

    def width(a):
        return pl.ds(0, MAIN if a < 3 else 128)

    def shard(a, w, j, core, lo=0, size=SENT):
        return w.at[rows_at(j, core, lo, size), width(a)]

    staged = (gg_out, gu_out, gd_out)
    own_copies = [
        pltpu.make_async_copy(src.at[0], dst, loc_sem.at[a])
        for a, (src, dst) in enumerate(zip((wg_in, wu_in, wd_in), staged))
    ]
    for cp in own_copies:
        cp.start()
    meta[0:4, :] = ids[...].astype(F32)
    meta[4:8, :] = gates_in[...]

    def widen(ext, src, flagged):
        for k in range(8):
            ext[CHUNK * k : CHUNK * k + OWN, :] = src[OWN * k : OWN * (k + 1), :]
            live = lax.broadcasted_iota(jnp.int32, (CHUNK - OWN, TOK), 0) == 0
            flag = one_zero(live) if flagged and k == 0 else jnp.zeros((CHUNK - OWN, TOK), F32)
            ext[CHUNK * k + OWN : CHUNK * (k + 1), :] = flag.astype(BF16)

    for a, w in enumerate(weights):
        lanes = w.shape[1]
        for k in range(8):
            w[pl.ds(CHUNK * k + SENT, CHUNK - SENT), :] = jnp.zeros((CHUNK - SENT, lanes), BF16)
        w[rows_at(h, c, SENT - 8, 8), :] = jnp.zeros((8, lanes), BF16)
        if a < 3:
            own_copies[a].wait()
            w[rows_at(h, c, 0, OWN), :MAIN] = staged[a][:, :MAIN]
    wrem[rows_at(h, c, 0, OWN), :] = jnp.concatenate(
        [ref[:, MAIN:] for ref in staged] + [jnp.zeros((OWN, 128 - 3 * REST), BF16)], axis=1
    )

    me.await_greetings()

    zex = [
        remote(src, dst, zs.at[k], zr.at[k], me.partner)
        for k, (src, dst) in enumerate(((meta, zmeta), (tok_in, ztok), (cot_in, zcot)))
    ]
    for cp in zex:
        cp.start()

    def ag(a, k):
        w = weights[a]
        s, r = ags.at[a * 9 + k], agr.at[a * 9 + k]
        if k == 0:
            return remote(shard(a, w, h, c), shard(a, w, h, c), s, r, me.up)
        if k == 1:
            return remote(shard(a, w, h, c), shard(a, w, h, c), s, r, me.down)
        if k == 2:
            return remote(shard(a, w, h, c), shard(a, w, h, c), s, r, me.sibling)
        if k == 3:
            part = shard(a, w, up_j(3), c, 0, HALF)
            return remote(part, part, s, r, me.up)
        if k == 4:
            part = shard(a, w, up_j(1), c, HALF, SENT - HALF)
            return remote(part, part, s, r, me.down)
        if k in (5, 6):
            part = shard(a, w, up_j(3 if k == 5 else 1), c)
            return remote(part, part, s, r, me.sibling)
        part = shard(a, w, up_j(2), c, 0, HALF) if k == 7 else shard(a, w, up_j(2), c, HALF, SENT - HALF)
        return remote(part, part, s, r, me.sibling)

    def ag_in(a, k):
        w = weights[a]
        s, r = ags.at[a * 9 + k], agr.at[a * 9 + k]
        lo, size = 0, SENT
        if k == 0:
            j, core = up_j(3), c
        elif k == 1:
            j, core = up_j(1), c
        elif k == 2:
            j, core = h, 1 - c
        elif k == 3:
            j, core, size = up_j(2), c, HALF
        elif k == 4:
            j, core, lo, size = up_j(2), c, HALF, SENT - HALF
        elif k in (5, 6):
            j, core = up_j(3 if k == 5 else 1), 1 - c
        elif k == 7:
            j, core, size = up_j(2), 1 - c, HALF
        else:
            j, core, lo, size = up_j(2), 1 - c, HALF, SENT - HALF
        part = shard(a, w, j, core, lo, size)
        return remote(part, part, s, r, me.sibling)

    for a in (3, 0, 1):
        for k in (0, 1, 2):
            ag(a, k).start()

    def dispatch_copy(bi, i, incoming):
        p, px, py = me.plane(i, -1 if incoming else 1)
        at = (bi * 16 + p) * SLOT
        source = me.block(px, py, bi) if incoming else me.block(me.x, me.y, bi)
        copies = []
        for arr, (src, dst) in enumerate(((send_x, recv_x), (send_g, recv_g))):
            k = (bi * 2 + arr) * 16 + i
            copies.append(
                remote(
                    src.at[pl.ds(mul(at, 8), SLOT), :],
                    dst.at[rows_of(source), :],
                    dss.at[k],
                    dsr.at[k],
                    me.plane_device(px, py),
                )
            )
        return copies

    def dispatch(bi, m_ref, t_ref, c_ref):
        place = lax.broadcasted_iota(jnp.int32, (16, TOK), 0)
        expert = ((place // 4) * 8 + me.zl * 4 + place % 4).astype(F32)
        named = jnp.zeros((16, TOK), F32)
        gates = jnp.zeros((16, TOK), F32)
        for k in range(4):
            hit = m_ref[k : k + 1, :] == expert
            named = named + one_zero(hit)
            gates = gates + jnp.where(hit, m_ref[4 + k : 5 + k, :], 0.0)
        earlier = one_zero(
            lax.broadcasted_iota(jnp.int32, (TOK, TOK), 0) < lax.broadcasted_iota(jnp.int32, (TOK, TOK), 1)
        ).astype(BF16)
        rank = dot(named.astype(BF16), earlier)
        rank = jnp.where(named > 0.5, rank, -1.0)
        slot = lax.broadcasted_iota(jnp.int32, (16, SLOT, TOK), 1).astype(F32)
        chosen3 = one_zero(slot == rank[:, None, :])
        weighted = (chosen3 * gates[:, None, :]).reshape(PLANE, TOK)
        pick = chosen3.reshape(PLANE, TOK).astype(BF16)
        mt[bi] = weighted
        slot_gate = jnp.sum(weighted, axis=1, keepdims=True)
        send_x[pl.ds(bi * PLANE, PLANE), :] = dot_nt(pick, t_ref[...]).astype(BF16)
        send_g[pl.ds(bi * PLANE, PLANE), :] = (dot_nt(pick, c_ref[...]) * slot_gate).astype(BF16)
        mine = rows_of(me.block(me.x, me.y, bi))
        here = pl.ds(mul((bi * 16 + me.p) * SLOT, 8), SLOT)
        recv_x[mine, :] = send_x[here, :]
        recv_g[mine, :] = send_g[here, :]

        @pl.loop(1, 16)
        def _(i):
            for cp in dispatch_copy(bi, i, False):
                cp.start()

    widen(tok, tok_in, True)
    widen(cot, cot_in, False)
    dispatch(0, meta, tok, cot)
    for cp in zex:
        cp.wait_recv()
    widen(tok, ztok, True)
    widen(cot, zcot, False)
    dispatch(1, zmeta, tok, cot)

    def forward_neighbours(a):
        ag_in(a, 0).wait_recv()
        ag(a, 3).start()
        ag(a, 5).start()
        ag_in(a, 1).wait_recv()
        ag(a, 4).start()
        ag(a, 6).start()

    forward_neighbours(3)
    forward_neighbours(0)
    forward_neighbours(1)
    for k in (0, 1, 2):
        ag(2, k).start()

    for bi in range(2):

        @pl.loop(1, 16)
        def _(i):
            for cp in dispatch_copy(bi, i, True):
                cp.wait_recv()

    eye_lane = one_zero(lax.broadcasted_iota(jnp.int32, (8, 128), 1) == OWN - 128).astype(BF16)
    flags = dot_nt(eye_lane, recv_x[:, 128:256])
    before = one_zero(
        lax.broadcasted_iota(jnp.int32, (SLOTS, SLOTS), 0) < lax.broadcasted_iota(jnp.int32, (SLOTS, SLOTS), 1)
    ).astype(BF16)
    position = dot(flags.astype(BF16), before)
    position = jnp.where(flags > 0.5, position, -1.0)[0:1, :]

    @pl.loop(0, 2)
    def _(m):
        at = mul(m * 256, 256)
        row = (lax.broadcasted_iota(jnp.int32, (256, SLOTS), 0) + at).astype(F32)
        pick = one_zero(row == position).astype(BF16)
        r_mat[pl.ds(at, 256), :] = pick
        x[pl.ds(at, 256), :] = dot(pick, recv_x[...]).astype(BF16)
        g[pl.ds(at, 256), :] = dot(pick, recv_g[...]).astype(BF16)

    def project(j, first):
        cols = pl.ds(mul(j * PAIR, 128), PAIR)
        rest = wrem[cols, :].astype(F32)
        lane = lax.broadcasted_iota(jnp.int32, (PAIR, 128), 1)
        for a in range(3):
            own = rest if a == 0 else pltpu.roll(rest, 128 - REST * a, 1)
            weights[a][cols, MAIN:] = jnp.where(lane < REST, own, 0.0).astype(BF16)

        @pl.loop(0, 2)
        def _(m):
            rows = pl.ds(mul(m * 256, 256), 256)
            xs = x[rows, cols]
            for acc, w in ((acc_g, wg), (acc_u, wu)):
                part = dot(xs, w[cols, :])
                acc[rows, :] = part if first else acc[rows, :] + part

    for a in (3, 0, 1):
        ag_in(a, 2).wait_recv()
    project(h, True)
    for a in (3, 0, 1):
        ag_in(a, 5).wait_recv()
    project(up_j(3), False)
    for a in (3, 0, 1):
        ag_in(a, 6).wait_recv()
    project(up_j(1), False)

    def finish_gather(a):
        ag_in(a, 3).wait_recv()
        ag(a, 7).start()
        ag_in(a, 4).wait_recv()
        ag(a, 8).start()

    def wait_opposite(a):
        ag_in(a, 7).wait_recv()
        ag_in(a, 8).wait_recv()

    for a in (3, 0, 1):
        finish_gather(a)
    for a in (3, 0, 1):
        wait_opposite(a)
    project(up_j(2), False)

    @pl.loop(0, 16)
    def _(m):
        rows = pl.ds(mul(m * 32, 32), 32)
        gate, up = acc_g[rows, :], acc_u[rows, :] + 1.0
        sg = jax.nn.sigmoid(SWISH_SLOPE * gate)
        value = gate * sg
        slope = sg + SWISH_SLOPE * value * (1.0 - sg)
        hid[rows, :] = (value * up).astype(BF16)
        acc_g[rows, :] = up * slope
        acc_u[rows, :] = value

    arrays = ((pd, g, hid), (wg, x, dg), (wu, x, du), (grem, None, None))

    def ra(a, k):
        if a in (0, 3):
            return (ra_d if a == 0 else ra_rem).at[k]
        return (recv_x, recv_g)[a - 1].at[pl.ds(CHUNK * k, SENT), width(a)]

    def half_in(a, lo, size):
        return hr.at[a, pl.ds(lo, size), :] if a < 3 else hr_rem.at[pl.ds(lo, size), :]

    def full_in(a, k):
        return fr.at[a * 2 + k] if a < 3 else fr_rem.at[k]

    def exchange(a, k):
        return remote(
            shard(a, arrays[a][0], up_j(k), 1 - c), ra(a, k), d2s.at[a * 4 + k], d2r.at[a * 4 + k], me.sibling
        )

    def parts_of(a, ks):
        parts, left, right = arrays[a]
        for k in ks:
            cols = pl.ds(mul(up_j(k) * PAIR, 128), PAIR)
            part = dot_tn(left[:, cols], right[...])
            parts[cols, :MAIN] = part[:, :MAIN].astype(BF16)
            exchange(a, k).start()
            rest = part[:, MAIN:]
            if a > 0:
                rest = grem[cols, :].astype(F32) + pltpu.roll(rest, REST * a, 1)
            grem[cols, :] = rest.astype(BF16)
            if a == 2:
                exchange(3, k).start()

    def half(a, k):
        lo, size = ((0, HALF), (HALF, SENT - HALF))[k]
        return remote(
            shard(a, arrays[a][0], up_j(2), c, lo, size),
            half_in(a, lo, size),
            hss.at[a * 2 + k],
            hsr.at[a * 2 + k],
            (me.up, me.down)[k],
        )

    def full(a, k):
        return remote(
            shard(a, arrays[a][0], up_j((1, 3)[k]), c),
            full_in(a, k),
            fss.at[a * 2 + k],
            fsr.at[a * 2 + k],
            (me.up, me.down)[k],
        )

    def send_halves(a):
        exchange(a, 2).wait_recv()
        at = rows_at(up_j(2), c), width(a)
        parts = arrays[a][0]
        parts[at] = (parts[at].astype(F32) + ra(a, 2)[...].astype(F32)).astype(BF16)
        half(a, 0).start()
        half(a, 1).start()

    def send_fulls(a):
        parts = arrays[a][0]
        for k, jj in ((0, 1), (1, 3)):
            exchange(a, jj).wait_recv()
            half(a, k).wait_recv()
            for with_half in (True, False):
                lo, size = ((0, HALF), (HALF, SENT - HALF))[k if with_half else 1 - k]
                at = rows_at(up_j(jj), c, lo, size), width(a)
                total = parts[at].astype(F32) + ra(a, jj)[lo : lo + size, :].astype(F32)
                if with_half:
                    total = total + half_in(a, lo, size)[...].astype(F32)
                parts[at] = total.astype(BF16)
            full(a, k).start()

    def down_step(j, first):
        cols = pl.ds(mul(j * PAIR, 128), PAIR)

        @pl.loop(0, 2)
        def _(m):
            rows = pl.ds(mul(m * 256, 256), 256)
            part = dot(g[rows, cols], wd[cols, :])
            acc_d[rows, :] = part if first else acc_d[rows, :] + part

    def out_step(j):
        cols = pl.ds(mul(j * PAIR, 128), PAIR)

        @pl.loop(0, 2)
        def _(m):
            rows = pl.ds(mul(m * 256, 256), 256)
            eo[rows, cols] = dot_nt(hid[rows, :], wd[cols, :]).astype(BF16)

    parts_of(0, (2, 1, 3, 0))
    for cp in zex:
        cp.wait_send()
    for bi in range(2):

        @pl.loop(1, 16)
        def _(i):
            for cp in dispatch_copy(bi, i, False):
                cp.wait_send()

    for a in (3, 0, 1):
        for k in range(9):
            ag(a, k).wait_send()
    send_halves(0)
    forward_neighbours(2)
    ag_in(2, 2).wait_recv()
    down_step(h, True)
    out_step(h)
    ag_in(2, 5).wait_recv()
    down_step(up_j(3), False)
    ag_in(2, 6).wait_recv()
    down_step(up_j(1), False)
    send_fulls(0)
    finish_gather(2)
    wait_opposite(2)
    down_step(up_j(2), False)

    @pl.loop(0, 16)
    def _(m):
        rows = pl.ds(mul(m * 32, 32), 32)
        dh = acc_d[rows, :]
        dg[rows, :] = (dh * acc_g[rows, :]).astype(BF16)
        du[rows, :] = (dh * acc_u[rows, :]).astype(BF16)

    parts_of(1, (2, 1))
    send_halves(1)
    parts_of(1, (3, 0))
    parts_of(2, (2, 1))
    send_halves(2)
    send_halves(3)
    parts_of(2, (3, 0))
    for k in (3, 1, 2):
        out_step(up_j(k))

    def back_copy(bi, i, incoming):
        p, px, py = me.plane(i, -1 if incoming else 1)
        place = p if incoming else me.p
        k = bi * 16 + i
        return remote(
            rets.at[rows_of(me.block(px, py, bi)), :],
            rr.at[pl.ds(mul((bi * 16 + place) * SLOT, 8), SLOT), :],
            rs.at[k],
            rr_sem.at[k],
            me.plane_device(px, py),
        )

    @pl.loop(0, 2)
    def _(m):
        cols = pl.ds(mul(m * PLANE, 128), PLANE)
        rets[pl.ds(mul(m * PLANE, 8), PLANE), :] = dot_tn(r_mat[:, cols], eo[...]).astype(BF16)

    send_fulls(1)
    for bi in range(2):
        rr[pl.ds(mul((bi * 16 + me.p) * SLOT, 8), SLOT), :] = rets[rows_of(me.block(me.x, me.y, bi)), :]

        @pl.loop(1, 16)
        def _(i):
            back_copy(bi, i, False).start()

    for bi in range(2):

        @pl.loop(1, 16)
        def _(i):
            back_copy(bi, i, True).wait_recv()

    def combine(bi):
        weight = mt[bi]
        high = weight.astype(BF16)
        low = (weight - high.astype(F32)).astype(BF16)
        both = dot_tn(rr[pl.ds(bi * PLANE, PLANE), :], jnp.concatenate([high, low], axis=1))
        return both[:, :TOK] + both[:, TOK:]

    theirs = combine(1).astype(BF16)
    for k in range(8):
        zsend[OWN * k : OWN * (k + 1), :] = theirs[CHUNK * k : CHUNK * k + OWN, :]
    zcopy = remote(zsend, zrecv, zs.at[3], zr.at[3], me.partner)
    zcopy.start()
    send_fulls(2)
    send_fulls(3)
    own = combine(0)
    zcopy.wait_recv()
    for k in range(8):
        at = slice(OWN * k, OWN * (k + 1))
        mixed_out[at, :] = (own[CHUNK * k : CHUNK * k + OWN, :] + zrecv[at, :].astype(F32)).astype(BF16)

    for a in range(4):
        exchange(a, 0).wait_recv()
        total = arrays[a][0][rows_at(h, c), width(a)].astype(F32) + ra(a, 0)[...].astype(F32)
        for k in range(2):
            full(a, k).wait_recv()
            total = total + full_in(a, k)[...].astype(F32)
        if a < 3:
            outs[a][:, :MAIN] = total.astype(BF16)[:OWN]
        else:
            for b in range(3):
                own = total if b == 0 else pltpu.roll(total, 128 - REST * b, 1)
                outs[b][:, MAIN:] = own.astype(BF16)[:OWN, :REST]

    zcopy.wait_send()
    for k in range(9):
        ag(2, k).wait_send()
    for a in range(4):
        for k in range(4):
            exchange(a, k).wait_send()
        for k in range(2):
            half(a, k).wait_send()
            full(a, k).wait_send()
    for bi in range(2):

        @pl.loop(1, 16)
        def _(i):
            back_copy(bi, i, False).wait_send()


def copy_kernel(*refs):
    srcs, dsts, held, (sem_in, sem_out) = refs[:4], refs[4:8], refs[8:12], refs[12:]
    loads = [pltpu.make_async_copy(s, v, sem_in.at[i]) for i, (s, v) in enumerate(zip(srcs, held))]
    stores = [pltpu.make_async_copy(v, d, sem_out.at[i]) for i, (v, d) in enumerate(zip(held, dsts))]
    for load in loads:
        load.start()
    for load, store in zip(loads, stores):
        load.wait()
        store.start()
    for store in stores:
        store.wait()


def body(tokens, cotangent, expert_ids, gate_weights, w_gate, w_up, w_down):
    dma = pltpu.SemaphoreType.DMA
    b16 = lambda *shape: pltpu.VMEM(shape, BF16)
    f32 = lambda *shape: pltpu.VMEM(shape, F32)
    results = [jax.ShapeDtypeStruct((OWN, FH), BF16)] * 3 + [jax.ShapeDtypeStruct((D, TOK), BF16)]
    anywhere = pl.BlockSpec(memory_space=pl.ANY)
    outs = pl.pallas_call(
        step_kernel,
        name="step",
        out_shape=results,
        in_specs=[VM()] * 4 + [anywhere] * 3,
        out_specs=[VM()] * 4,
        scratch_shapes=[
            b16(DP, DP), b16(DP, DP), b16(DP, DP), b16(DP, 128), b16(DP, 128),
            b16(4, SENT, 128), b16(SENT, 128), b16(2, SENT, 128),
            f32(8, TOK), f32(8, TOK), b16(DP, TOK), b16(DP, TOK), b16(D, TOK), b16(D, TOK),
            b16(SLOTS, DP), b16(SLOTS, DP), b16(SLOTS, DP), b16(SLOTS, DP),
            b16(CAP, DP), b16(CAP, DP), b16(CAP, DP), b16(CAP, DP),
            f32(CAP, DP), f32(CAP, DP), f32(CAP, DP),
            b16(DP, DP), b16(4, SENT, MAIN), b16(3, SENT, MAIN), b16(6, SENT, MAIN),
            b16(SLOTS, DP), b16(SLOTS, DP), b16(CAP, SLOTS), f32(2, PLANE, TOK), b16(D, TOK), b16(D, TOK),
            dma((3,)), dma((4,)), dma((4,)), dma((36,)), dma((36,)), dma((64,)), dma((64,)),
            dma((16,)), dma((16,)), dma((8,)), dma((8,)), dma((8,)), dma((8,)), dma((32,)), dma((32,)),
        ],
        compiler_params=pltpu.CompilerParams(
            collective_id=0, has_side_effects=True, vmem_limit_bytes=67043328
        ),
    )(expert_ids.T, gate_weights.T, tokens.T, cotangent.T, w_gate, w_up, w_down)
    gg, gu, gd, mixed = pl.pallas_call(
        copy_kernel,
        name="results",
        out_shape=results,
        in_specs=[anywhere] * 4,
        out_specs=[anywhere] * 4,
        scratch_shapes=[b16(*r.shape) for r in results] + [dma((4,)), dma((4,))],
    )(*outs)
    return mixed.T, gg[None], gu[None], gd[None]


def solution(mesh):
    rows, weight = P(("expert", "dp"), None), P("expert", "dp", None)
    return jax.shard_map(
        body,
        mesh=mesh,
        in_specs=(rows, rows, rows, rows, weight, weight, weight),
        out_specs=(rows, weight, weight, weight),
        check_vma=False,
    )
```

```python
import functools

import jax
import jax.numpy as jnp
from jax import lax
from jax.experimental import pallas as pl
from jax.experimental.pallas import tpu as pltpu
from jax.sharding import PartitionSpec as P

MESH = pl.DeviceIdType.MESH
SWISH_SLOPE = 1.702
F32, BF16 = jnp.float32, jnp.bfloat16
TOK = 128
CAP = 512
SLOT = 24
D = 1440
FH = 1440
OWN = 180
SENT = 176
TAIL = OWN - SENT
CHUNK = 192
DP = 8 * CHUNK
PAIR = 2 * CHUNK
MAIN = 1408
REST = FH - MAIN
TILES = MAIN // 128
MISC = OWN + 3 * TILES * TAIL
MISC_HALF = 160
HALF = 88
SLOTS = 32 * SLOT
PLANE = 16 * SLOT
VM = functools.partial(pl.BlockSpec, memory_space=pltpu.VMEM)


def mul(value, k):
    return pl.multiple_of(value, k)


class Place:
    def __init__(self):
        e, d = lax.axis_index("expert"), lax.axis_index("dp")
        self.x, self.zl, self.y = e // 8, (e // 4) % 2, e % 4
        self.h, self.c = d // 2, d % 2
        self.e, self.d = e, d
        self.sibling = (e, self.h * 2 + 1 - self.c)
        self.up = (e, ((self.h + 1) % 4) * 2 + self.c)
        self.down = (e, ((self.h + 3) % 4) * 2 + self.c)
        self.partner = (self.x * 8 + (1 - self.zl) * 4 + self.y, d)
        self.p = self.x * 4 + self.y

    def plane(self, i, sign):
        px = (self.x + sign * (i // 4) + 4) % 4
        py = (self.y + sign * (i % 4) + 4) % 4
        return px * 4 + py, px, py

    def plane_device(self, px, py):
        return (px * 8 + self.zl * 4 + py, self.d)

    def block(self, px, py, bi):
        zb = self.zl if bi == 0 else 1 - self.zl
        return px * 8 + zb * 4 + py

    def greet(self):
        barrier = pltpu.get_barrier_semaphore()
        for peer in (self.sibling, self.up, self.down, self.partner):
            pl.semaphore_signal(barrier, inc=1, device_id=peer, device_id_type=MESH)

        @pl.loop(1, 16)
        def _(i):
            _, px, py = self.plane(i, 1)
            pl.semaphore_signal(
                barrier, inc=1, device_id=self.plane_device(px, py), device_id_type=MESH
            )

    def await_greetings(self):
        pl.semaphore_wait(pltpu.get_barrier_semaphore(), 19)


def remote(src, dst, ssem, rsem, device):
    return pltpu.make_async_remote_copy(
        src_ref=src, dst_ref=dst, send_sem=ssem, recv_sem=rsem, device_id=device, device_id_type=MESH
    )


def rows_of(block, size=SLOT):
    return pl.ds(mul(block * SLOT, 8), size)


def dot(a, b):
    return jnp.dot(a, b, preferred_element_type=F32)


def dot_nt(a, b):
    return lax.dot_general(a, b, (((1,), (1,)), ((), ())), preferred_element_type=F32)


def dot_tn(a, b):
    return lax.dot_general(a, b, (((0,), (0,)), ((), ())), preferred_element_type=F32)


def one_zero(flag):
    return jnp.where(flag, 1.0, 0.0)


def step_kernel(
    ids, gates_in, tok_in, cot_in, wg_in, wu_in, wd_in,
    gg_out, gu_out, gd_out, mixed_out,
    wg, wu, wd, wrem, grem, ra_rem, hr_rem, fr_rem, meta, zmeta, tok, cot, ztok, zcot, send_x, send_g, recv_x, recv_g,
    x, g, hid, eo, acc_g, acc_u, acc_d, pd, ra_d, hr, fr, rets, rr, r_mat, mt, zsend, zrecv,
    loc_sem, zs, zr, ags, agr, dss, dsr, d2s, d2r, hss, hsr, fss, fsr, rs, rr_sem,
):
    me = Place()
    me.greet()
    h, c = me.h, me.c
    weights = (wg, wu, wd, wrem)
    outs = (gd_out, gg_out, gu_out)
    dg, du = send_x.at[pl.ds(0, CAP), :], send_g.at[pl.ds(0, CAP), :]

    def up_j(k):
        return (h + k) % 4

    def base(j, core):
        return CHUNK * (2 * j + core)

    def rows_at(j, core, lo=0, size=SENT):
        return pl.ds(mul(base(j, core) + lo, 8), size)

    def misc_at(j, core, lo=0, size=MISC):
        return pl.ds(mul(MISC * (2 * j + core) + lo, 8), size)

    def span(a, half=None):
        rows, first = (SENT, HALF) if a < 3 else (MISC, MISC_HALF)
        return (0, rows) if half is None else ((0, first), (first, rows - first))[half]

    def place_of(a, j, core, half=None):
        lo, size = span(a, half)
        return (rows_at if a < 3 else misc_at)(j, core, lo, size), width(a)

    def width(a):
        return pl.ds(0, MAIN if a < 3 else 128)

    def shard(a, w, j, core, half=None):
        return w.at[place_of(a, j, core, half)]

    staged = (gg_out, gu_out, gd_out)
    own_copies = [
        pltpu.make_async_copy(src.at[0], dst, loc_sem.at[a])
        for a, (src, dst) in enumerate(zip((wg_in, wu_in, wd_in), staged))
    ]
    for cp in own_copies:
        cp.start()
    meta[0:4, :] = ids[...].astype(F32)
    meta[4:8, :] = gates_in[...]

    def widen(ext, src, flagged):
        for k in range(8):
            ext[CHUNK * k : CHUNK * k + OWN, :] = src[OWN * k : OWN * (k + 1), :]
            live = lax.broadcasted_iota(jnp.int32, (CHUNK - OWN, TOK), 0) == 0
            flag = one_zero(live) if flagged and k == 0 else jnp.zeros((CHUNK - OWN, TOK), F32)
            ext[CHUNK * k + OWN : CHUNK * (k + 1), :] = flag.astype(BF16)

    for a, w in enumerate(weights[:3]):
        for k in range(8):
            w[pl.ds(CHUNK * k + SENT, CHUNK - SENT), :] = jnp.zeros((CHUNK - SENT, DP), BF16)
        own_copies[a].wait()
        w[rows_at(h, c), :MAIN] = staged[a][:SENT, :MAIN]
    last_lanes = jnp.concatenate(
        [ref[:, MAIN:].astype(F32) for ref in staged] + [jnp.zeros((OWN, 128 - 3 * REST), F32)], axis=1
    )
    last_rows = [
        ref[SENT:, 128 * t : 128 * (t + 1)].astype(F32) for ref in staged for t in range(TILES)
    ]
    wrem[misc_at(h, c), :] = jnp.concatenate([last_lanes, *last_rows], axis=0).astype(BF16)

    me.await_greetings()

    zex = [
        remote(src, dst, zs.at[k], zr.at[k], me.partner)
        for k, (src, dst) in enumerate(((meta, zmeta), (tok_in, ztok), (cot_in, zcot)))
    ]
    for cp in zex:
        cp.start()

    def ag(a, k):
        w = weights[a]
        s, r = ags.at[a * 9 + k], agr.at[a * 9 + k]
        if k == 0:
            return remote(shard(a, w, h, c), shard(a, w, h, c), s, r, me.up)
        if k == 1:
            return remote(shard(a, w, h, c), shard(a, w, h, c), s, r, me.down)
        if k == 2:
            return remote(shard(a, w, h, c), shard(a, w, h, c), s, r, me.sibling)
        if k == 3:
            part = shard(a, w, up_j(3), c, 0)
            return remote(part, part, s, r, me.up)
        if k == 4:
            part = shard(a, w, up_j(1), c, 1)
            return remote(part, part, s, r, me.down)
        if k in (5, 6):
            part = shard(a, w, up_j(3 if k == 5 else 1), c)
            return remote(part, part, s, r, me.sibling)
        part = shard(a, w, up_j(2), c, k - 7)
        return remote(part, part, s, r, me.sibling)

    def ag_in(a, k):
        w = weights[a]
        s, r = ags.at[a * 9 + k], agr.at[a * 9 + k]
        half = None
        if k == 0:
            j, core = up_j(3), c
        elif k == 1:
            j, core = up_j(1), c
        elif k == 2:
            j, core = h, 1 - c
        elif k in (3, 4):
            j, core, half = up_j(2), c, k - 3
        elif k in (5, 6):
            j, core = up_j(3 if k == 5 else 1), 1 - c
        else:
            j, core, half = up_j(2), 1 - c, k - 7
        part = shard(a, w, j, core, half)
        return remote(part, part, s, r, me.sibling)

    for a in (3, 0, 1):
        for k in (0, 1, 2):
            ag(a, k).start()

    def dispatch_copy(bi, i, incoming):
        p, px, py = me.plane(i, -1 if incoming else 1)
        at = (bi * 16 + p) * SLOT
        source = me.block(px, py, bi) if incoming else me.block(me.x, me.y, bi)
        copies = []
        for arr, (src, dst) in enumerate(((send_x, recv_x), (send_g, recv_g))):
            k = (bi * 2 + arr) * 16 + i
            copies.append(
                remote(
                    src.at[pl.ds(mul(at, 8), SLOT), :],
                    dst.at[rows_of(source), :],
                    dss.at[k],
                    dsr.at[k],
                    me.plane_device(px, py),
                )
            )
        return copies

    def dispatch(bi, m_ref, t_ref, c_ref):
        place = lax.broadcasted_iota(jnp.int32, (16, TOK), 0)
        expert = ((place // 4) * 8 + me.zl * 4 + place % 4).astype(F32)
        named = jnp.zeros((16, TOK), F32)
        gates = jnp.zeros((16, TOK), F32)
        for k in range(4):
            hit = m_ref[k : k + 1, :] == expert
            named = named + one_zero(hit)
            gates = gates + jnp.where(hit, m_ref[4 + k : 5 + k, :], 0.0)
        earlier = one_zero(
            lax.broadcasted_iota(jnp.int32, (TOK, TOK), 0) < lax.broadcasted_iota(jnp.int32, (TOK, TOK), 1)
        ).astype(BF16)
        rank = dot(named.astype(BF16), earlier)
        rank = jnp.where(named > 0.5, rank, -1.0)
        slot = lax.broadcasted_iota(jnp.int32, (16, SLOT, TOK), 1).astype(F32)
        chosen3 = one_zero(slot == rank[:, None, :])
        weighted = (chosen3 * gates[:, None, :]).reshape(PLANE, TOK)
        pick = chosen3.reshape(PLANE, TOK).astype(BF16)
        mt[bi] = weighted
        slot_gate = jnp.sum(weighted, axis=1, keepdims=True)
        send_x[pl.ds(bi * PLANE, PLANE), :] = dot_nt(pick, t_ref[...]).astype(BF16)
        send_g[pl.ds(bi * PLANE, PLANE), :] = (dot_nt(pick, c_ref[...]) * slot_gate).astype(BF16)
        mine = rows_of(me.block(me.x, me.y, bi))
        here = pl.ds(mul((bi * 16 + me.p) * SLOT, 8), SLOT)
        recv_x[mine, :] = send_x[here, :]
        recv_g[mine, :] = send_g[here, :]

        @pl.loop(1, 16)
        def _(i):
            for cp in dispatch_copy(bi, i, False):
                cp.start()

    widen(tok, tok_in, True)
    widen(cot, cot_in, False)
    dispatch(0, meta, tok, cot)
    for cp in zex:
        cp.wait_recv()
    widen(tok, ztok, True)
    widen(cot, zcot, False)
    dispatch(1, zmeta, tok, cot)

    def forward_neighbours(a):
        ag_in(a, 0).wait_recv()
        ag(a, 3).start()
        ag(a, 5).start()
        ag_in(a, 1).wait_recv()
        ag(a, 4).start()
        ag(a, 6).start()

    forward_neighbours(3)
    forward_neighbours(0)
    forward_neighbours(1)
    for k in (0, 1, 2):
        ag(2, k).start()

    for bi in range(2):

        @pl.loop(1, 16)
        def _(i):
            for cp in dispatch_copy(bi, i, True):
                cp.wait_recv()

    eye_lane = one_zero(lax.broadcasted_iota(jnp.int32, (8, 128), 1) == OWN - 128).astype(BF16)
    flags = dot_nt(eye_lane, recv_x[:, 128:256])
    before = one_zero(
        lax.broadcasted_iota(jnp.int32, (SLOTS, SLOTS), 0) < lax.broadcasted_iota(jnp.int32, (SLOTS, SLOTS), 1)
    ).astype(BF16)
    position = dot(flags.astype(BF16), before)
    position = jnp.where(flags > 0.5, position, -1.0)[0:1, :]

    @pl.loop(0, 2)
    def _(m):
        at = mul(m * 256, 256)
        row = (lax.broadcasted_iota(jnp.int32, (256, SLOTS), 0) + at).astype(F32)
        pick = one_zero(row == position).astype(BF16)
        r_mat[pl.ds(at, 256), :] = pick
        x[pl.ds(at, 256), :] = dot(pick, recv_x[...]).astype(BF16)
        g[pl.ds(at, 256), :] = dot(pick, recv_g[...]).astype(BF16)

    def project(j, first):
        cols = pl.ds(mul(j * PAIR, 128), PAIR)
        live = lax.broadcasted_iota(jnp.int32, (SENT + 8, 128), 0) < OWN
        live = live & (lax.broadcasted_iota(jnp.int32, (SENT + 8, 128), 1) < REST)
        for core in range(2):
            misc = wrem[misc_at(j, core), :].astype(F32)
            rest = misc[: SENT + 8]
            for a in range(3):
                own = rest if a == 0 else pltpu.roll(rest, 128 - REST * a, 1)
                weights[a][rows_at(j, core, 0, SENT + 8), MAIN:] = jnp.where(live, own, 0.0).astype(BF16)
                for t in range(TILES):
                    at = OWN + TAIL * (a * TILES + t)
                    last = jnp.concatenate([misc[at : at + TAIL], jnp.zeros((8 - TAIL, 128), F32)], axis=0)
                    weights[a][rows_at(j, core, SENT, 8), 128 * t : 128 * (t + 1)] = last.astype(BF16)

        @pl.loop(0, 2)
        def _(m):
            rows = pl.ds(mul(m * 256, 256), 256)
            xs = x[rows, cols]
            for acc, w in ((acc_g, wg), (acc_u, wu)):
                part = dot(xs, w[cols, :])
                acc[rows, :] = part if first else acc[rows, :] + part

    for a in (3, 0, 1):
        ag_in(a, 2).wait_recv()
    project(h, True)
    for a in (3, 0, 1):
        ag_in(a, 5).wait_recv()
    project(up_j(3), False)
    for a in (3, 0, 1):
        ag_in(a, 6).wait_recv()
    project(up_j(1), False)

    def finish_gather(a):
        ag_in(a, 3).wait_recv()
        ag(a, 7).start()
        ag_in(a, 4).wait_recv()
        ag(a, 8).start()

    def wait_opposite(a):
        ag_in(a, 7).wait_recv()
        ag_in(a, 8).wait_recv()

    for a in (3, 0, 1):
        finish_gather(a)
    for a in (3, 0, 1):
        wait_opposite(a)
    project(up_j(2), False)

    @pl.loop(0, 16)
    def _(m):
        rows = pl.ds(mul(m * 32, 32), 32)
        gate, up = acc_g[rows, :], acc_u[rows, :] + 1.0
        sg = jax.nn.sigmoid(SWISH_SLOPE * gate)
        value = gate * sg
        slope = sg + SWISH_SLOPE * value * (1.0 - sg)
        hid[rows, :] = (value * up).astype(BF16)
        acc_g[rows, :] = up * slope
        acc_u[rows, :] = value

    arrays = ((pd, g, hid), (wg, x, dg), (wu, x, du), (grem, None, None))

    def ra(a, k):
        if a in (0, 3):
            return (ra_d if a == 0 else ra_rem).at[k]
        return (recv_x, recv_g)[a - 1].at[pl.ds(CHUNK * k, SENT), width(a)]

    def half_in(a, k):
        rows = pl.ds(*span(a, k))
        return hr.at[a, rows, :] if a < 3 else hr_rem.at[rows, :]

    def full_in(a, k):
        return fr.at[a * 2 + k] if a < 3 else fr_rem.at[k]

    def exchange(a, k):
        return remote(
            shard(a, arrays[a][0], up_j(k), 1 - c), ra(a, k), d2s.at[a * 4 + k], d2r.at[a * 4 + k], me.sibling
        )

    def parts_of(a, ks):
        parts, left, right = arrays[a]
        for k in ks:
            cols = pl.ds(mul(up_j(k) * PAIR, 128), PAIR)
            part = dot_tn(left[:, cols], right[...])
            parts[cols, :MAIN] = part[:, :MAIN].astype(BF16)
            exchange(a, k).start()
            for core in range(2):
                own = part[CHUNK * core : CHUNK * core + OWN]
                rest = own[:, MAIN:] if a == 0 else pltpu.roll(own[:, MAIN:], REST * a, 1)
                pieces = [rest]
                if a > 0:
                    pieces.append(jnp.zeros((a * TILES * TAIL, 128), F32))
                pieces += [own[SENT:, 128 * t : 128 * (t + 1)] for t in range(TILES)]
                if a < 2:
                    pieces.append(jnp.zeros(((2 - a) * TILES * TAIL, 128), F32))
                misc = jnp.concatenate(pieces, axis=0)
                at = misc_at(up_j(k), core)
                if a > 0:
                    misc = misc + grem[at, :].astype(F32)
                grem[at, :] = misc.astype(BF16)
            if a == 2:
                exchange(3, k).start()

    def half(a, k):
        return remote(
            shard(a, arrays[a][0], up_j(2), c, k),
            half_in(a, k),
            hss.at[a * 2 + k],
            hsr.at[a * 2 + k],
            (me.up, me.down)[k],
        )

    def full(a, k):
        return remote(
            shard(a, arrays[a][0], up_j((1, 3)[k]), c),
            full_in(a, k),
            fss.at[a * 2 + k],
            fsr.at[a * 2 + k],
            (me.up, me.down)[k],
        )

    def send_halves(a):
        exchange(a, 2).wait_recv()
        at = place_of(a, up_j(2), c)
        parts = arrays[a][0]
        parts[at] = (parts[at].astype(F32) + ra(a, 2)[...].astype(F32)).astype(BF16)
        half(a, 0).start()
        half(a, 1).start()

    def send_fulls(a):
        parts = arrays[a][0]
        for k, jj in ((0, 1), (1, 3)):
            exchange(a, jj).wait_recv()
            half(a, k).wait_recv()
            for with_half in (True, False):
                side = k if with_half else 1 - k
                at = place_of(a, up_j(jj), c, side)
                total = parts[at].astype(F32) + ra(a, jj)[pl.ds(*span(a, side)), :].astype(F32)
                if with_half:
                    total = total + half_in(a, k)[...].astype(F32)
                parts[at] = total.astype(BF16)
            full(a, k).start()

    def down_step(j, first):
        cols = pl.ds(mul(j * PAIR, 128), PAIR)

        @pl.loop(0, 2)
        def _(m):
            rows = pl.ds(mul(m * 256, 256), 256)
            part = dot(g[rows, cols], wd[cols, :])
            acc_d[rows, :] = part if first else acc_d[rows, :] + part

    def out_step(j):
        cols = pl.ds(mul(j * PAIR, 128), PAIR)

        @pl.loop(0, 2)
        def _(m):
            rows = pl.ds(mul(m * 256, 256), 256)
            eo[rows, cols] = dot_nt(hid[rows, :], wd[cols, :]).astype(BF16)

    parts_of(0, (2, 1, 3, 0))
    for cp in zex:
        cp.wait_send()
    for bi in range(2):

        @pl.loop(1, 16)
        def _(i):
            for cp in dispatch_copy(bi, i, False):
                cp.wait_send()

    for a in (3, 0, 1):
        for k in range(9):
            ag(a, k).wait_send()
    forward_neighbours(2)
    send_halves(0)
    ag_in(2, 2).wait_recv()
    down_step(h, True)
    out_step(h)
    ag_in(2, 5).wait_recv()
    down_step(up_j(3), False)
    ag_in(2, 6).wait_recv()
    down_step(up_j(1), False)
    finish_gather(2)
    wait_opposite(2)
    down_step(up_j(2), False)

    @pl.loop(0, 16)
    def _(m):
        rows = pl.ds(mul(m * 32, 32), 32)
        dh = acc_d[rows, :]
        dg[rows, :] = (dh * acc_g[rows, :]).astype(BF16)
        du[rows, :] = (dh * acc_u[rows, :]).astype(BF16)

    parts_of(1, (2, 1))
    send_halves(1)
    send_fulls(0)
    parts_of(1, (3, 0))
    parts_of(2, (2, 1))
    send_halves(2)
    send_halves(3)
    parts_of(2, (3, 0))
    for k in (3, 1, 2):
        out_step(up_j(k))

    def back_copy(bi, i, incoming):
        p, px, py = me.plane(i, -1 if incoming else 1)
        place = p if incoming else me.p
        k = bi * 16 + i
        return remote(
            rets.at[rows_of(me.block(px, py, bi)), :],
            rr.at[pl.ds(mul((bi * 16 + place) * SLOT, 8), SLOT), :],
            rs.at[k],
            rr_sem.at[k],
            me.plane_device(px, py),
        )

    @pl.loop(0, 2)
    def _(m):
        cols = pl.ds(mul(m * PLANE, 128), PLANE)
        rets[pl.ds(mul(m * PLANE, 8), PLANE), :] = dot_tn(r_mat[:, cols], eo[...]).astype(BF16)

    send_fulls(1)
    for bi in range(2):
        rr[pl.ds(mul((bi * 16 + me.p) * SLOT, 8), SLOT), :] = rets[rows_of(me.block(me.x, me.y, bi)), :]

        @pl.loop(1, 16)
        def _(i):
            back_copy(bi, i, False).start()

    for bi in range(2):

        @pl.loop(1, 16)
        def _(i):
            back_copy(bi, i, True).wait_recv()

    def combine(bi):
        weight = mt[bi]
        high = weight.astype(BF16)
        low = (weight - high.astype(F32)).astype(BF16)
        both = dot_tn(rr[pl.ds(bi * PLANE, PLANE), :], jnp.concatenate([high, low], axis=1))
        return both[:, :TOK] + both[:, TOK:]

    theirs = combine(1).astype(BF16)
    for k in range(8):
        zsend[OWN * k : OWN * (k + 1), :] = theirs[CHUNK * k : CHUNK * k + OWN, :]
    zcopy = remote(zsend, zrecv, zs.at[3], zr.at[3], me.partner)
    zcopy.start()
    send_fulls(2)
    send_fulls(3)
    own = combine(0)
    zcopy.wait_recv()
    for k in range(8):
        at = slice(OWN * k, OWN * (k + 1))
        mixed_out[at, :] = (own[CHUNK * k : CHUNK * k + OWN, :] + zrecv[at, :].astype(F32)).astype(BF16)

    for k in range(9):
        ag(2, k).wait_send()
    for a in range(4):
        for k in range(4):
            exchange(a, k).wait_send()
        for k in range(2):
            half(a, k).wait_send()
    for bi in range(2):

        @pl.loop(1, 16)
        def _(i):
            back_copy(bi, i, False).wait_send()

    for a in range(4):
        exchange(a, 0).wait_recv()
        total = arrays[a][0][place_of(a, h, c)].astype(F32) + ra(a, 0)[...].astype(F32)
        for k in range(2):
            full(a, k).wait_recv()
            total = total + full_in(a, k)[...].astype(F32)
        if a < 3:
            outs[a][:SENT, :MAIN] = total.astype(BF16)
        else:
            for b in range(3):
                own = total[:OWN] if b == 0 else pltpu.roll(total[:OWN], 128 - REST * b, 1)
                outs[b][:, MAIN:] = own.astype(BF16)[:, :REST]
                for t in range(TILES):
                    at = OWN + TAIL * (b * TILES + t)
                    outs[b][SENT:, 128 * t : 128 * (t + 1)] = total[at : at + TAIL].astype(BF16)

    zcopy.wait_send()
    for a in range(4):
        for k in range(2):
            full(a, k).wait_send()


def copy_kernel(*refs):
    srcs, dsts, held, (sem_in, sem_out) = refs[:4], refs[4:8], refs[8:12], refs[12:]
    loads = [pltpu.make_async_copy(s, v, sem_in.at[i]) for i, (s, v) in enumerate(zip(srcs, held))]
    stores = [pltpu.make_async_copy(v, d, sem_out.at[i]) for i, (v, d) in enumerate(zip(held, dsts))]
    for load in loads:
        load.start()
    for load, store in zip(loads, stores):
        load.wait()
        store.start()
    for store in stores:
        store.wait()


def body(tokens, cotangent, expert_ids, gate_weights, w_gate, w_up, w_down):
    dma = pltpu.SemaphoreType.DMA
    b16 = lambda *shape: pltpu.VMEM(shape, BF16)
    f32 = lambda *shape: pltpu.VMEM(shape, F32)
    results = [jax.ShapeDtypeStruct((OWN, FH), BF16)] * 3 + [jax.ShapeDtypeStruct((D, TOK), BF16)]
    anywhere = pl.BlockSpec(memory_space=pl.ANY)
    outs = pl.pallas_call(
        step_kernel,
        name="step",
        out_shape=results,
        in_specs=[VM()] * 4 + [anywhere] * 3,
        out_specs=[VM()] * 4,
        scratch_shapes=[
            b16(DP, DP), b16(DP, DP), b16(DP, DP), b16(8 * MISC, 128), b16(8 * MISC, 128),
            b16(4, MISC, 128), b16(MISC, 128), b16(2, MISC, 128),
            f32(8, TOK), f32(8, TOK), b16(DP, TOK), b16(DP, TOK), b16(D, TOK), b16(D, TOK),
            b16(SLOTS, DP), b16(SLOTS, DP), b16(SLOTS, DP), b16(SLOTS, DP),
            b16(CAP, DP), b16(CAP, DP), b16(CAP, DP), b16(CAP, DP),
            f32(CAP, DP), f32(CAP, DP), f32(CAP, DP),
            b16(DP, DP), b16(4, SENT, MAIN), b16(3, SENT, MAIN), b16(6, SENT, MAIN),
            b16(SLOTS, DP), b16(SLOTS, DP), b16(CAP, SLOTS), f32(2, PLANE, TOK), b16(D, TOK), b16(D, TOK),
            dma((3,)), dma((4,)), dma((4,)), dma((36,)), dma((36,)), dma((64,)), dma((64,)),
            dma((16,)), dma((16,)), dma((8,)), dma((8,)), dma((8,)), dma((8,)), dma((32,)), dma((32,)),
        ],
        compiler_params=pltpu.CompilerParams(
            collective_id=0, has_side_effects=True, vmem_limit_bytes=67043328
        ),
    )(expert_ids.T, gate_weights.T, tokens.T, cotangent.T, w_gate, w_up, w_down)
    gg, gu, gd, mixed = pl.pallas_call(
        copy_kernel,
        name="results",
        out_shape=results,
        in_specs=[anywhere] * 4,
        out_specs=[anywhere] * 4,
        scratch_shapes=[b16(*r.shape) for r in results] + [dma((4,)), dma((4,))],
    )(*outs)
    return mixed.T, gg[None], gu[None], gd[None]


def solution(mesh):
    rows, weight = P(("expert", "dp"), None), P("expert", "dp", None)
    return jax.shard_map(
        body,
        mesh=mesh,
        in_specs=(rows, rows, rows, rows, weight, weight, weight),
        out_specs=(rows, weight, weight, weight),
        check_vma=False,
    )
```

```python
import functools

import jax
import jax.numpy as jnp
from jax import lax
from jax.experimental import pallas as pl
from jax.experimental.pallas import tpu as pltpu
from jax.sharding import PartitionSpec as P

MESH = pl.DeviceIdType.MESH
SWISH_SLOPE = 1.702
F32, BF16 = jnp.float32, jnp.bfloat16
TOK = 128
CAP = 512
SLOT = 24
D = 1440
FH = 1440
OWN = 180
SENT = 176
TAIL = OWN - SENT
CHUNK = 192
DP = 8 * CHUNK
PAIR = 2 * CHUNK
MAIN = 1408
REST = FH - MAIN
TILES = MAIN // 128
MISC = OWN + 3 * TILES * TAIL
MISC_HALF = 160
HALF = 88
SLOTS = 32 * SLOT
PLANE = 16 * SLOT
VM = functools.partial(pl.BlockSpec, memory_space=pltpu.VMEM)


def mul(value, k):
    return pl.multiple_of(value, k)


class Place:
    def __init__(self):
        e, d = lax.axis_index("expert"), lax.axis_index("dp")
        self.x, self.zl, self.y = e // 8, (e // 4) % 2, e % 4
        self.h, self.c = d // 2, d % 2
        self.e, self.d = e, d
        self.sibling = (e, self.h * 2 + 1 - self.c)
        self.up = (e, ((self.h + 1) % 4) * 2 + self.c)
        self.down = (e, ((self.h + 3) % 4) * 2 + self.c)
        self.partner = (self.x * 8 + (1 - self.zl) * 4 + self.y, d)
        self.p = self.x * 4 + self.y

    def plane(self, i, sign):
        px = (self.x + sign * (i // 4) + 4) % 4
        py = (self.y + sign * (i % 4) + 4) % 4
        return px * 4 + py, px, py

    def plane_device(self, px, py):
        return (px * 8 + self.zl * 4 + py, self.d)

    def block(self, px, py, bi):
        zb = self.zl if bi == 0 else 1 - self.zl
        return px * 8 + zb * 4 + py

    def greet(self):
        barrier = pltpu.get_barrier_semaphore()
        for peer in (self.sibling, self.up, self.down, self.partner):
            pl.semaphore_signal(barrier, inc=1, device_id=peer, device_id_type=MESH)

        @pl.loop(1, 16)
        def _(i):
            _, px, py = self.plane(i, 1)
            pl.semaphore_signal(
                barrier, inc=1, device_id=self.plane_device(px, py), device_id_type=MESH
            )

    def await_greetings(self):
        pl.semaphore_wait(pltpu.get_barrier_semaphore(), 19)


def remote(src, dst, ssem, rsem, device):
    return pltpu.make_async_remote_copy(
        src_ref=src, dst_ref=dst, send_sem=ssem, recv_sem=rsem, device_id=device, device_id_type=MESH
    )


def rows_of(block, size=SLOT):
    return pl.ds(mul(block * SLOT, 8), size)


def dot(a, b):
    return jnp.dot(a, b, preferred_element_type=F32)


def dot_nt(a, b):
    return lax.dot_general(a, b, (((1,), (1,)), ((), ())), preferred_element_type=F32)


def dot_tn(a, b):
    return lax.dot_general(a, b, (((0,), (0,)), ((), ())), preferred_element_type=F32)


def one_zero(flag):
    return jnp.where(flag, 1.0, 0.0)


def step_kernel(
    ids_hbm, gates_hbm, tok_hbm, cot_hbm, wg_in, wu_in, wd_in,
    gg_out, gu_out, gd_out, mixed_out,
    ids, gates_in, tok_in, cot_in, wg, wu, wd, wrem, grem, ra_rem, hr_rem, fr_rem, meta, zmeta, tok, cot, ztok, zcot, send_x, send_g, recv_x, recv_g,
    x, g, hid, eo, acc_g, acc_u, acc_d, pd, ra_d, hr, fr, rets, rr, r_mat, mt, zsend, zrecv,
    loc_sem, zs, zr, ags, agr, dss, dsr, d2s, d2r, hss, hsr, fss, fsr, rs, rr_sem,
):
    me = Place()
    me.greet()
    h, c = me.h, me.c
    weights = (wg, wu, wd, wrem)
    outs = (gd_out, gg_out, gu_out)
    dg, du = send_x.at[pl.ds(0, CAP), :], send_g.at[pl.ds(0, CAP), :]

    def up_j(k):
        return (h + k) % 4

    def base(j, core):
        return CHUNK * (2 * j + core)

    def rows_at(j, core, lo=0, size=SENT):
        return pl.ds(mul(base(j, core) + lo, 8), size)

    def misc_at(j, core, lo=0, size=MISC):
        return pl.ds(mul(MISC * (2 * j + core) + lo, 8), size)

    def span(a, half=None):
        rows, first = (SENT, HALF) if a < 3 else (MISC, MISC_HALF)
        return (0, rows) if half is None else ((0, first), (first, rows - first))[half]

    def place_of(a, j, core, half=None):
        lo, size = span(a, half)
        return (rows_at if a < 3 else misc_at)(j, core, lo, size), width(a)

    def width(a):
        return pl.ds(0, MAIN if a < 3 else 128)

    def shard(a, w, j, core, half=None):
        return w.at[place_of(a, j, core, half)]

    staged = (gg_out, gu_out, gd_out)
    own_copies = [
        pltpu.make_async_copy(src.at[0], dst, loc_sem.at[a])
        for a, (src, dst) in enumerate(zip((wg_in, wu_in, wd_in), staged))
    ]
    for cp in own_copies:
        cp.start()
    inputs = [
        pltpu.make_async_copy(src, dst, loc_sem.at[3 + k])
        for k, (src, dst) in enumerate(
            ((ids_hbm, ids), (gates_hbm, gates_in), (tok_hbm, tok_in), (cot_hbm, cot_in))
        )
    ]
    for cp in inputs:
        cp.start()
    for cp in inputs[:2]:
        cp.wait()
    meta[0:4, :] = ids[...].astype(F32)
    meta[4:8, :] = gates_in[...]

    def widen(ext, src, flagged):
        for k in range(8):
            ext[CHUNK * k : CHUNK * k + OWN, :] = src[OWN * k : OWN * (k + 1), :]
            live = lax.broadcasted_iota(jnp.int32, (CHUNK - OWN, TOK), 0) == 0
            flag = one_zero(live) if flagged and k == 0 else jnp.zeros((CHUNK - OWN, TOK), F32)
            ext[CHUNK * k + OWN : CHUNK * (k + 1), :] = flag.astype(BF16)

    for a, w in enumerate(weights[:3]):
        for k in range(8):
            w[pl.ds(CHUNK * k + SENT, CHUNK - SENT), :] = jnp.zeros((CHUNK - SENT, DP), BF16)
        own_copies[a].wait()
        w[rows_at(h, c), :MAIN] = staged[a][:SENT, :MAIN]
    last_lanes = jnp.concatenate(
        [ref[:, MAIN:].astype(F32) for ref in staged] + [jnp.zeros((OWN, 128 - 3 * REST), F32)], axis=1
    )
    last_rows = [
        ref[SENT:, 128 * t : 128 * (t + 1)].astype(F32) for ref in staged for t in range(TILES)
    ]
    wrem[misc_at(h, c), :] = jnp.concatenate([last_lanes, *last_rows], axis=0).astype(BF16)

    for cp in inputs[2:]:
        cp.wait()
    me.await_greetings()

    zex = [
        remote(src, dst, zs.at[k], zr.at[k], me.partner)
        for k, (src, dst) in enumerate(((meta, zmeta), (tok_in, ztok), (cot_in, zcot)))
    ]
    for cp in zex:
        cp.start()

    def ag(a, k):
        w = weights[a]
        s, r = ags.at[a * 9 + k], agr.at[a * 9 + k]
        if k == 0:
            return remote(shard(a, w, h, c), shard(a, w, h, c), s, r, me.up)
        if k == 1:
            return remote(shard(a, w, h, c), shard(a, w, h, c), s, r, me.down)
        if k == 2:
            return remote(shard(a, w, h, c), shard(a, w, h, c), s, r, me.sibling)
        if k == 3:
            part = shard(a, w, up_j(3), c, 0)
            return remote(part, part, s, r, me.up)
        if k == 4:
            part = shard(a, w, up_j(1), c, 1)
            return remote(part, part, s, r, me.down)
        if k in (5, 6):
            part = shard(a, w, up_j(3 if k == 5 else 1), c)
            return remote(part, part, s, r, me.sibling)
        part = shard(a, w, up_j(2), c, k - 7)
        return remote(part, part, s, r, me.sibling)

    def ag_in(a, k):
        w = weights[a]
        s, r = ags.at[a * 9 + k], agr.at[a * 9 + k]
        half = None
        if k == 0:
            j, core = up_j(3), c
        elif k == 1:
            j, core = up_j(1), c
        elif k == 2:
            j, core = h, 1 - c
        elif k in (3, 4):
            j, core, half = up_j(2), c, k - 3
        elif k in (5, 6):
            j, core = up_j(3 if k == 5 else 1), 1 - c
        else:
            j, core, half = up_j(2), 1 - c, k - 7
        part = shard(a, w, j, core, half)
        return remote(part, part, s, r, me.sibling)

    for a in (3, 0, 1):
        for k in (0, 1, 2):
            ag(a, k).start()

    def dispatch_copy(bi, i, incoming):
        p, px, py = me.plane(i, -1 if incoming else 1)
        at = (bi * 16 + p) * SLOT
        source = me.block(px, py, bi) if incoming else me.block(me.x, me.y, bi)
        copies = []
        for arr, (src, dst) in enumerate(((send_x, recv_x), (send_g, recv_g))):
            k = (bi * 2 + arr) * 16 + i
            copies.append(
                remote(
                    src.at[pl.ds(mul(at, 8), SLOT), :],
                    dst.at[rows_of(source), :],
                    dss.at[k],
                    dsr.at[k],
                    me.plane_device(px, py),
                )
            )
        return copies

    def dispatch(bi, m_ref, t_ref, c_ref):
        place = lax.broadcasted_iota(jnp.int32, (16, TOK), 0)
        expert = ((place // 4) * 8 + me.zl * 4 + place % 4).astype(F32)
        named = jnp.zeros((16, TOK), F32)
        gates = jnp.zeros((16, TOK), F32)
        for k in range(4):
            hit = m_ref[k : k + 1, :] == expert
            named = named + one_zero(hit)
            gates = gates + jnp.where(hit, m_ref[4 + k : 5 + k, :], 0.0)
        earlier = one_zero(
            lax.broadcasted_iota(jnp.int32, (TOK, TOK), 0) < lax.broadcasted_iota(jnp.int32, (TOK, TOK), 1)
        ).astype(BF16)
        rank = dot(named.astype(BF16), earlier)
        rank = jnp.where(named > 0.5, rank, -1.0)
        slot = lax.broadcasted_iota(jnp.int32, (16, SLOT, TOK), 1).astype(F32)
        chosen3 = one_zero(slot == rank[:, None, :])
        weighted = (chosen3 * gates[:, None, :]).reshape(PLANE, TOK)
        pick = chosen3.reshape(PLANE, TOK).astype(BF16)
        mt[bi] = weighted
        slot_gate = jnp.sum(weighted, axis=1, keepdims=True)
        send_x[pl.ds(bi * PLANE, PLANE), :] = dot_nt(pick, t_ref[...]).astype(BF16)
        send_g[pl.ds(bi * PLANE, PLANE), :] = (dot_nt(pick, c_ref[...]) * slot_gate).astype(BF16)
        mine = rows_of(me.block(me.x, me.y, bi))
        here = pl.ds(mul((bi * 16 + me.p) * SLOT, 8), SLOT)
        recv_x[mine, :] = send_x[here, :]
        recv_g[mine, :] = send_g[here, :]

        @pl.loop(1, 16)
        def _(i):
            for cp in dispatch_copy(bi, i, False):
                cp.start()

    widen(tok, tok_in, True)
    widen(cot, cot_in, False)
    dispatch(0, meta, tok, cot)
    for cp in zex:
        cp.wait_recv()
    widen(tok, ztok, True)
    widen(cot, zcot, False)
    dispatch(1, zmeta, tok, cot)

    def forward_neighbours(a):
        ag_in(a, 0).wait_recv()
        ag(a, 3).start()
        ag(a, 5).start()
        ag_in(a, 1).wait_recv()
        ag(a, 4).start()
        ag(a, 6).start()

    forward_neighbours(3)
    forward_neighbours(0)
    forward_neighbours(1)
    for k in (0, 1, 2):
        ag(2, k).start()

    for bi in range(2):

        @pl.loop(1, 16)
        def _(i):
            for cp in dispatch_copy(bi, i, True):
                cp.wait_recv()

    eye_lane = one_zero(lax.broadcasted_iota(jnp.int32, (8, 128), 1) == OWN - 128).astype(BF16)
    flags = dot_nt(eye_lane, recv_x[:, 128:256])
    before = one_zero(
        lax.broadcasted_iota(jnp.int32, (SLOTS, SLOTS), 0) < lax.broadcasted_iota(jnp.int32, (SLOTS, SLOTS), 1)
    ).astype(BF16)
    position = dot(flags.astype(BF16), before)
    position = jnp.where(flags > 0.5, position, -1.0)[0:1, :]

    @pl.loop(0, 2)
    def _(m):
        at = mul(m * 256, 256)
        row = (lax.broadcasted_iota(jnp.int32, (256, SLOTS), 0) + at).astype(F32)
        pick = one_zero(row == position).astype(BF16)
        r_mat[pl.ds(at, 256), :] = pick
        x[pl.ds(at, 256), :] = dot(pick, recv_x[...]).astype(BF16)
        g[pl.ds(at, 256), :] = dot(pick, recv_g[...]).astype(BF16)

    def project(j, first):
        cols = pl.ds(mul(j * PAIR, 128), PAIR)
        live = lax.broadcasted_iota(jnp.int32, (SENT + 8, 128), 0) < OWN
        live = live & (lax.broadcasted_iota(jnp.int32, (SENT + 8, 128), 1) < REST)
        for core in range(2):
            misc = wrem[misc_at(j, core), :].astype(F32)
            rest = misc[: SENT + 8]
            for a in range(3):
                own = rest if a == 0 else pltpu.roll(rest, 128 - REST * a, 1)
                weights[a][rows_at(j, core, 0, SENT + 8), MAIN:] = jnp.where(live, own, 0.0).astype(BF16)
                for t in range(TILES):
                    at = OWN + TAIL * (a * TILES + t)
                    last = jnp.concatenate([misc[at : at + TAIL], jnp.zeros((8 - TAIL, 128), F32)], axis=0)
                    weights[a][rows_at(j, core, SENT, 8), 128 * t : 128 * (t + 1)] = last.astype(BF16)

        @pl.loop(0, 2)
        def _(m):
            rows = pl.ds(mul(m * 256, 256), 256)
            xs = x[rows, cols]
            for acc, w in ((acc_g, wg), (acc_u, wu)):
                part = dot(xs, w[cols, :])
                acc[rows, :] = part if first else acc[rows, :] + part

    for a in (3, 0, 1):
        ag_in(a, 2).wait_recv()
    project(h, True)
    for a in (3, 0, 1):
        ag_in(a, 5).wait_recv()
    project(up_j(3), False)
    for a in (3, 0, 1):
        ag_in(a, 6).wait_recv()
    project(up_j(1), False)

    def finish_gather(a):
        ag_in(a, 3).wait_recv()
        ag(a, 7).start()
        ag_in(a, 4).wait_recv()
        ag(a, 8).start()

    def wait_opposite(a):
        ag_in(a, 7).wait_recv()
        ag_in(a, 8).wait_recv()

    for a in (3, 0, 1):
        finish_gather(a)
    for a in (3, 0, 1):
        wait_opposite(a)
    project(up_j(2), False)

    @pl.loop(0, 16)
    def _(m):
        rows = pl.ds(mul(m * 32, 32), 32)
        gate, up = acc_g[rows, :], acc_u[rows, :] + 1.0
        sg = jax.nn.sigmoid(SWISH_SLOPE * gate)
        value = gate * sg
        slope = sg + SWISH_SLOPE * value * (1.0 - sg)
        hid[rows, :] = (value * up).astype(BF16)
        acc_g[rows, :] = up * slope
        acc_u[rows, :] = value

    arrays = ((pd, g, hid), (wg, x, dg), (wu, x, du), (grem, None, None))

    def ra(a, k):
        if a in (0, 3):
            return (ra_d if a == 0 else ra_rem).at[k]
        return (recv_x, recv_g)[a - 1].at[pl.ds(CHUNK * k, SENT), width(a)]

    def half_in(a, k):
        rows = pl.ds(*span(a, k))
        return hr.at[a, rows, :] if a < 3 else hr_rem.at[rows, :]

    def full_in(a, k):
        return fr.at[a * 2 + k] if a < 3 else fr_rem.at[k]

    def exchange(a, k):
        return remote(
            shard(a, arrays[a][0], up_j(k), 1 - c), ra(a, k), d2s.at[a * 4 + k], d2r.at[a * 4 + k], me.sibling
        )

    def parts_of(a, ks):
        parts, left, right = arrays[a]
        for k in ks:
            cols = pl.ds(mul(up_j(k) * PAIR, 128), PAIR)
            part = dot_tn(left[:, cols], right[...])
            parts[cols, :MAIN] = part[:, :MAIN].astype(BF16)
            exchange(a, k).start()
            for core in range(2):
                own = part[CHUNK * core : CHUNK * core + OWN]
                rest = own[:, MAIN:] if a == 0 else pltpu.roll(own[:, MAIN:], REST * a, 1)
                pieces = [rest]
                if a > 0:
                    pieces.append(jnp.zeros((a * TILES * TAIL, 128), F32))
                pieces += [own[SENT:, 128 * t : 128 * (t + 1)] for t in range(TILES)]
                if a < 2:
                    pieces.append(jnp.zeros(((2 - a) * TILES * TAIL, 128), F32))
                misc = jnp.concatenate(pieces, axis=0)
                at = misc_at(up_j(k), core)
                if a > 0:
                    misc = misc + grem[at, :].astype(F32)
                grem[at, :] = misc.astype(BF16)
            if a == 2:
                exchange(3, k).start()

    def half(a, k):
        return remote(
            shard(a, arrays[a][0], up_j(2), c, k),
            half_in(a, k),
            hss.at[a * 2 + k],
            hsr.at[a * 2 + k],
            (me.up, me.down)[k],
        )

    def full(a, k):
        return remote(
            shard(a, arrays[a][0], up_j((1, 3)[k]), c),
            full_in(a, k),
            fss.at[a * 2 + k],
            fsr.at[a * 2 + k],
            (me.up, me.down)[k],
        )

    def send_halves(a):
        exchange(a, 2).wait_recv()
        at = place_of(a, up_j(2), c)
        parts = arrays[a][0]
        parts[at] = (parts[at].astype(F32) + ra(a, 2)[...].astype(F32)).astype(BF16)
        half(a, 0).start()
        half(a, 1).start()

    def send_fulls(a):
        parts = arrays[a][0]
        for k, jj in ((0, 1), (1, 3)):
            exchange(a, jj).wait_recv()
            half(a, k).wait_recv()
            for with_half in (True, False):
                side = k if with_half else 1 - k
                at = place_of(a, up_j(jj), c, side)
                total = parts[at].astype(F32) + ra(a, jj)[pl.ds(*span(a, side)), :].astype(F32)
                if with_half:
                    total = total + half_in(a, k)[...].astype(F32)
                parts[at] = total.astype(BF16)
            full(a, k).start()

    def down_step(j, first):
        cols = pl.ds(mul(j * PAIR, 128), PAIR)

        @pl.loop(0, 2)
        def _(m):
            rows = pl.ds(mul(m * 256, 256), 256)
            part = dot(g[rows, cols], wd[cols, :])
            acc_d[rows, :] = part if first else acc_d[rows, :] + part

    def out_step(j):
        cols = pl.ds(mul(j * PAIR, 128), PAIR)

        @pl.loop(0, 2)
        def _(m):
            rows = pl.ds(mul(m * 256, 256), 256)
            eo[rows, cols] = dot_nt(hid[rows, :], wd[cols, :]).astype(BF16)

    parts_of(0, (2, 1, 3, 0))
    for cp in zex:
        cp.wait_send()
    for bi in range(2):

        @pl.loop(1, 16)
        def _(i):
            for cp in dispatch_copy(bi, i, False):
                cp.wait_send()

    for a in (3, 0, 1):
        for k in range(9):
            ag(a, k).wait_send()
    forward_neighbours(2)
    send_halves(0)
    ag_in(2, 2).wait_recv()
    down_step(h, True)
    out_step(h)
    ag_in(2, 5).wait_recv()
    down_step(up_j(3), False)
    ag_in(2, 6).wait_recv()
    down_step(up_j(1), False)
    finish_gather(2)
    wait_opposite(2)
    down_step(up_j(2), False)

    @pl.loop(0, 16)
    def _(m):
        rows = pl.ds(mul(m * 32, 32), 32)
        dh = acc_d[rows, :]
        dg[rows, :] = (dh * acc_g[rows, :]).astype(BF16)
        du[rows, :] = (dh * acc_u[rows, :]).astype(BF16)

    parts_of(1, (2, 1))
    send_halves(1)
    parts_of(1, (3, 0))
    parts_of(2, (2, 1))
    send_halves(2)
    send_halves(3)
    send_fulls(0)
    parts_of(2, (3, 0))
    for k in (3, 1, 2):
        out_step(up_j(k))

    def back_copy(bi, i, incoming):
        p, px, py = me.plane(i, -1 if incoming else 1)
        place = p if incoming else me.p
        k = bi * 16 + i
        return remote(
            rets.at[rows_of(me.block(px, py, bi)), :],
            rr.at[pl.ds(mul((bi * 16 + place) * SLOT, 8), SLOT), :],
            rs.at[k],
            rr_sem.at[k],
            me.plane_device(px, py),
        )

    @pl.loop(0, 2)
    def _(m):
        cols = pl.ds(mul(m * PLANE, 128), PLANE)
        rets[pl.ds(mul(m * PLANE, 8), PLANE), :] = dot_tn(r_mat[:, cols], eo[...]).astype(BF16)

    send_fulls(1)
    for bi in range(2):
        rr[pl.ds(mul((bi * 16 + me.p) * SLOT, 8), SLOT), :] = rets[rows_of(me.block(me.x, me.y, bi)), :]

        @pl.loop(1, 16)
        def _(i):
            back_copy(bi, i, False).start()

    for bi in range(2):

        @pl.loop(1, 16)
        def _(i):
            back_copy(bi, i, True).wait_recv()

    def combine(bi):
        weight = mt[bi]
        high = weight.astype(BF16)
        low = (weight - high.astype(F32)).astype(BF16)
        both = dot_tn(rr[pl.ds(bi * PLANE, PLANE), :], jnp.concatenate([high, low], axis=1))
        return both[:, :TOK] + both[:, TOK:]

    theirs = combine(1).astype(BF16)
    for k in range(8):
        zsend[OWN * k : OWN * (k + 1), :] = theirs[CHUNK * k : CHUNK * k + OWN, :]
    zcopy = remote(zsend, zrecv, zs.at[3], zr.at[3], me.partner)
    zcopy.start()
    send_fulls(2)
    send_fulls(3)
    own = combine(0)
    zcopy.wait_recv()
    for k in range(8):
        at = slice(OWN * k, OWN * (k + 1))
        mixed_out[at, :] = (own[CHUNK * k : CHUNK * k + OWN, :] + zrecv[at, :].astype(F32)).astype(BF16)

    for k in range(9):
        ag(2, k).wait_send()
    for a in range(4):
        for k in range(4):
            exchange(a, k).wait_send()
        for k in range(2):
            half(a, k).wait_send()
    for bi in range(2):

        @pl.loop(1, 16)
        def _(i):
            back_copy(bi, i, False).wait_send()

    for a in range(4):
        exchange(a, 0).wait_recv()
        total = arrays[a][0][place_of(a, h, c)].astype(F32) + ra(a, 0)[...].astype(F32)
        for k in range(2):
            full(a, k).wait_recv()
            total = total + full_in(a, k)[...].astype(F32)
        if a < 3:
            outs[a][:SENT, :MAIN] = total.astype(BF16)
        else:
            for b in range(3):
                own = total[:OWN] if b == 0 else pltpu.roll(total[:OWN], 128 - REST * b, 1)
                outs[b][:, MAIN:] = own.astype(BF16)[:, :REST]
                for t in range(TILES):
                    at = OWN + TAIL * (b * TILES + t)
                    outs[b][SENT:, 128 * t : 128 * (t + 1)] = total[at : at + TAIL].astype(BF16)

    zcopy.wait_send()
    for a in range(4):
        for k in range(2):
            full(a, k).wait_send()


def copy_kernel(*refs):
    srcs, dsts, held, (sem_in, sem_out) = refs[:4], refs[4:8], refs[8:12], refs[12:]
    loads = [pltpu.make_async_copy(s, v, sem_in.at[i]) for i, (s, v) in enumerate(zip(srcs, held))]
    stores = [pltpu.make_async_copy(v, d, sem_out.at[i]) for i, (v, d) in enumerate(zip(held, dsts))]
    for load in loads:
        load.start()
    for load, store in zip(loads, stores):
        load.wait()
        store.start()
    for store in stores:
        store.wait()


def body(tokens, cotangent, expert_ids, gate_weights, w_gate, w_up, w_down):
    dma = pltpu.SemaphoreType.DMA
    b16 = lambda *shape: pltpu.VMEM(shape, BF16)
    f32 = lambda *shape: pltpu.VMEM(shape, F32)
    results = [jax.ShapeDtypeStruct((OWN, FH), BF16)] * 3 + [jax.ShapeDtypeStruct((D, TOK), BF16)]
    anywhere = pl.BlockSpec(memory_space=pl.ANY)
    outs = pl.pallas_call(
        step_kernel,
        name="step",
        out_shape=results,
        in_specs=[anywhere] * 7,
        out_specs=[VM()] * 4,
        scratch_shapes=[
            pltpu.VMEM((4, TOK), jnp.int32), f32(4, TOK), b16(D, TOK), b16(D, TOK),
            b16(DP, DP), b16(DP, DP), b16(DP, DP), b16(8 * MISC, 128), b16(8 * MISC, 128),
            b16(4, MISC, 128), b16(MISC, 128), b16(2, MISC, 128),
            f32(8, TOK), f32(8, TOK), b16(DP, TOK), b16(DP, TOK), b16(D, TOK), b16(D, TOK),
            b16(SLOTS, DP), b16(SLOTS, DP), b16(SLOTS, DP), b16(SLOTS, DP),
            b16(CAP, DP), b16(CAP, DP), b16(CAP, DP), b16(CAP, DP),
            f32(CAP, DP), f32(CAP, DP), f32(CAP, DP),
            b16(DP, DP), b16(4, SENT, MAIN), b16(3, SENT, MAIN), b16(6, SENT, MAIN),
            b16(SLOTS, DP), b16(SLOTS, DP), b16(CAP, SLOTS), f32(2, PLANE, TOK), b16(D, TOK), b16(D, TOK),
            dma((7,)), dma((4,)), dma((4,)), dma((36,)), dma((36,)), dma((64,)), dma((64,)),
            dma((16,)), dma((16,)), dma((8,)), dma((8,)), dma((8,)), dma((8,)), dma((32,)), dma((32,)),
        ],
        compiler_params=pltpu.CompilerParams(
            collective_id=0, has_side_effects=True, vmem_limit_bytes=67043328
        ),
    )(expert_ids.T, gate_weights.T, tokens.T, cotangent.T, w_gate, w_up, w_down)
    gg, gu, gd, mixed = pl.pallas_call(
        copy_kernel,
        name="results",
        out_shape=results,
        in_specs=[anywhere] * 4,
        out_specs=[anywhere] * 4,
        scratch_shapes=[b16(*r.shape) for r in results] + [dma((4,)), dma((4,))],
    )(*outs)
    return mixed.T, gg[None], gu[None], gd[None]


def solution(mesh):
    rows, weight = P(("expert", "dp"), None), P("expert", "dp", None)
    return jax.shard_map(
        body,
        mesh=mesh,
        in_specs=(rows, rows, rows, rows, weight, weight, weight),
        out_specs=(rows, weight, weight, weight),
        check_vma=False,
    )
```

```python
import functools

import jax
import jax.numpy as jnp
from jax import lax
from jax.experimental import pallas as pl
from jax.experimental.pallas import tpu as pltpu
from jax.sharding import PartitionSpec as P

MESH = pl.DeviceIdType.MESH
SWISH_SLOPE = 1.702
F32, BF16 = jnp.float32, jnp.bfloat16
TOK = 128
CAP = 512
SLOT = 24
D = 1440
FH = 1440
OWN = 180
SENT = 176
TAIL = OWN - SENT
CHUNK = 192
DP = 8 * CHUNK
PAIR = 2 * CHUNK
MAIN = 1408
REST = FH - MAIN
TILES = MAIN // 128
MISC = OWN + 3 * TILES * TAIL
MISC_HALF = 160
HALF = 88
SLOTS = 32 * SLOT
PLANE = 16 * SLOT
VM = functools.partial(pl.BlockSpec, memory_space=pltpu.VMEM)


def mul(value, k):
    return pl.multiple_of(value, k)


class Place:
    def __init__(self):
        e, d = lax.axis_index("expert"), lax.axis_index("dp")
        self.x, self.zl, self.y = e // 8, (e // 4) % 2, e % 4
        self.h, self.c = d // 2, d % 2
        self.e, self.d = e, d
        self.sibling = (e, self.h * 2 + 1 - self.c)
        self.up = (e, ((self.h + 1) % 4) * 2 + self.c)
        self.down = (e, ((self.h + 3) % 4) * 2 + self.c)
        self.partner = (self.x * 8 + (1 - self.zl) * 4 + self.y, d)
        self.p = self.x * 4 + self.y

    def plane(self, i, sign):
        px = (self.x + sign * (i // 4) + 4) % 4
        py = (self.y + sign * (i % 4) + 4) % 4
        return px * 4 + py, px, py

    def plane_device(self, px, py):
        return (px * 8 + self.zl * 4 + py, self.d)

    def block(self, px, py, bi):
        zb = self.zl if bi == 0 else 1 - self.zl
        return px * 8 + zb * 4 + py

    def greet(self):
        barrier = pltpu.get_barrier_semaphore()
        for peer in (self.sibling, self.up, self.down, self.partner):
            pl.semaphore_signal(barrier, inc=1, device_id=peer, device_id_type=MESH)

        @pl.loop(1, 16)
        def _(i):
            _, px, py = self.plane(i, 1)
            pl.semaphore_signal(
                barrier, inc=1, device_id=self.plane_device(px, py), device_id_type=MESH
            )

    def await_greetings(self):
        pl.semaphore_wait(pltpu.get_barrier_semaphore(), 19)


def remote(src, dst, ssem, rsem, device):
    return pltpu.make_async_remote_copy(
        src_ref=src, dst_ref=dst, send_sem=ssem, recv_sem=rsem, device_id=device, device_id_type=MESH
    )


def rows_of(block, size=SLOT):
    return pl.ds(mul(block * SLOT, 8), size)


def dot(a, b):
    return jnp.dot(a, b, preferred_element_type=F32)


def dot_nt(a, b):
    return lax.dot_general(a, b, (((1,), (1,)), ((), ())), preferred_element_type=F32)


def dot_tn(a, b):
    return lax.dot_general(a, b, (((0,), (0,)), ((), ())), preferred_element_type=F32)


def one_zero(flag):
    return jnp.where(flag, 1.0, 0.0)


def step_kernel(
    ids_hbm, gates_hbm, tok_hbm, cot_hbm, wg_in, wu_in, wd_in,
    gg_out, gu_out, gd_out, mixed_out,
    ids, gates_in, tok_in, cot_in, wg, wu, wd, wrem, grem, ra_rem, hr_rem, fr_rem, meta, zmeta, tok, cot, ztok, zcot, send_x, send_g, recv_x, recv_g,
    x, g, hid, eo, acc_g, acc_u, acc_d, pd, ra_d, hr, fr, rets, rr, r_mat, mt, zsend, zrecv,
    loc_sem, zs, zr, ags, agr, dss, dsr, d2s, d2r, hss, hsr, fss, fsr, rs, rr_sem,
):
    me = Place()
    me.greet()
    h, c = me.h, me.c
    weights = (wg, wu, wd, wrem)
    outs = (gd_out, gg_out, gu_out)
    dg, du = send_x.at[pl.ds(0, CAP), :], send_g.at[pl.ds(0, CAP), :]

    def up_j(k):
        return (h + k) % 4

    def base(j, core):
        return CHUNK * (2 * j + core)

    def rows_at(j, core, lo=0, size=SENT):
        return pl.ds(mul(base(j, core) + lo, 8), size)

    def misc_at(j, core, lo=0, size=MISC):
        return pl.ds(mul(MISC * (2 * j + core) + lo, 8), size)

    def span(a, half=None):
        rows, first = (SENT, HALF) if a < 3 else (MISC, MISC_HALF)
        return (0, rows) if half is None else ((0, first), (first, rows - first))[half]

    def place_of(a, j, core, half=None):
        lo, size = span(a, half)
        return (rows_at if a < 3 else misc_at)(j, core, lo, size), width(a)

    def width(a):
        return pl.ds(0, MAIN if a < 3 else 128)

    def shard(a, w, j, core, half=None):
        return w.at[place_of(a, j, core, half)]

    staged = (gg_out, gu_out, gd_out)
    own_copies = [
        pltpu.make_async_copy(src.at[0], dst, loc_sem.at[a])
        for a, (src, dst) in enumerate(zip((wg_in, wu_in, wd_in), staged))
    ]
    for cp in own_copies:
        cp.start()
    inputs = [
        pltpu.make_async_copy(src, dst, loc_sem.at[3 + k])
        for k, (src, dst) in enumerate(
            ((ids_hbm, ids), (gates_hbm, gates_in), (tok_hbm, tok_in), (cot_hbm, cot_in))
        )
    ]
    for cp in inputs:
        cp.start()
    for cp in inputs[:2]:
        cp.wait()
    meta[0:4, :] = ids[...].astype(F32)
    meta[4:8, :] = gates_in[...]

    def widen(ext, src, flagged):
        for k in range(8):
            ext[CHUNK * k : CHUNK * k + OWN, :] = src[OWN * k : OWN * (k + 1), :]
            live = lax.broadcasted_iota(jnp.int32, (CHUNK - OWN, TOK), 0) == 0
            flag = one_zero(live) if flagged and k == 0 else jnp.zeros((CHUNK - OWN, TOK), F32)
            ext[CHUNK * k + OWN : CHUNK * (k + 1), :] = flag.astype(BF16)

    for a, w in enumerate(weights[:3]):
        for k in range(8):
            w[pl.ds(CHUNK * k + SENT, CHUNK - SENT), :] = jnp.zeros((CHUNK - SENT, DP), BF16)
        own_copies[a].wait()
        w[rows_at(h, c), :MAIN] = staged[a][:SENT, :MAIN]
    last_lanes = jnp.concatenate(
        [ref[:, MAIN:].astype(F32) for ref in staged] + [jnp.zeros((OWN, 128 - 3 * REST), F32)], axis=1
    )
    last_rows = [
        ref[SENT:, 128 * t : 128 * (t + 1)].astype(F32) for ref in staged for t in range(TILES)
    ]
    wrem[misc_at(h, c), :] = jnp.concatenate([last_lanes, *last_rows], axis=0).astype(BF16)

    for cp in inputs[2:]:
        cp.wait()
    me.await_greetings()

    zex = [
        remote(src, dst, zs.at[k], zr.at[k], me.partner)
        for k, (src, dst) in enumerate(((meta, zmeta), (tok_in, ztok), (cot_in, zcot)))
    ]
    for cp in zex:
        cp.start()

    def ag(a, k):
        w = weights[a]
        s, r = ags.at[a * 9 + k], agr.at[a * 9 + k]
        if k == 0:
            return remote(shard(a, w, h, c), shard(a, w, h, c), s, r, me.up)
        if k == 1:
            return remote(shard(a, w, h, c), shard(a, w, h, c), s, r, me.down)
        if k == 2:
            return remote(shard(a, w, h, c), shard(a, w, h, c), s, r, me.sibling)
        if k == 3:
            part = shard(a, w, up_j(3), c, 0)
            return remote(part, part, s, r, me.up)
        if k == 4:
            part = shard(a, w, up_j(1), c, 1)
            return remote(part, part, s, r, me.down)
        if k in (5, 6):
            part = shard(a, w, up_j(3 if k == 5 else 1), c)
            return remote(part, part, s, r, me.sibling)
        part = shard(a, w, up_j(2), c, k - 7)
        return remote(part, part, s, r, me.sibling)

    def ag_in(a, k):
        w = weights[a]
        s, r = ags.at[a * 9 + k], agr.at[a * 9 + k]
        half = None
        if k == 0:
            j, core = up_j(3), c
        elif k == 1:
            j, core = up_j(1), c
        elif k == 2:
            j, core = h, 1 - c
        elif k in (3, 4):
            j, core, half = up_j(2), c, k - 3
        elif k in (5, 6):
            j, core = up_j(3 if k == 5 else 1), 1 - c
        else:
            j, core, half = up_j(2), 1 - c, k - 7
        part = shard(a, w, j, core, half)
        return remote(part, part, s, r, me.sibling)

    for a in (3, 0, 1):
        for k in (0, 1, 2):
            ag(a, k).start()

    def dispatch_copy(bi, i, incoming):
        p, px, py = me.plane(i, -1 if incoming else 1)
        at = (bi * 16 + p) * SLOT
        source = me.block(px, py, bi) if incoming else me.block(me.x, me.y, bi)
        copies = []
        for arr, (src, dst) in enumerate(((send_x, recv_x), (send_g, recv_g))):
            k = (bi * 2 + arr) * 16 + i
            copies.append(
                remote(
                    src.at[pl.ds(mul(at, 8), SLOT), :],
                    dst.at[rows_of(source), :],
                    dss.at[k],
                    dsr.at[k],
                    me.plane_device(px, py),
                )
            )
        return copies

    def dispatch(bi, m_ref, t_ref, c_ref):
        place = lax.broadcasted_iota(jnp.int32, (16, TOK), 0)
        expert = ((place // 4) * 8 + me.zl * 4 + place % 4).astype(F32)
        named = jnp.zeros((16, TOK), F32)
        gates = jnp.zeros((16, TOK), F32)
        for k in range(4):
            hit = m_ref[k : k + 1, :] == expert
            named = named + one_zero(hit)
            gates = gates + jnp.where(hit, m_ref[4 + k : 5 + k, :], 0.0)
        earlier = one_zero(
            lax.broadcasted_iota(jnp.int32, (TOK, TOK), 0) < lax.broadcasted_iota(jnp.int32, (TOK, TOK), 1)
        ).astype(BF16)
        rank = dot(named.astype(BF16), earlier)
        rank = jnp.where(named > 0.5, rank, -1.0)
        slot = lax.broadcasted_iota(jnp.int32, (16, SLOT, TOK), 1).astype(F32)
        chosen3 = one_zero(slot == rank[:, None, :])
        weighted = (chosen3 * gates[:, None, :]).reshape(PLANE, TOK)
        pick = chosen3.reshape(PLANE, TOK).astype(BF16)
        mt[bi] = weighted
        slot_gate = jnp.sum(weighted, axis=1, keepdims=True)
        send_x[pl.ds(bi * PLANE, PLANE), :] = dot_nt(pick, t_ref[...]).astype(BF16)
        send_g[pl.ds(bi * PLANE, PLANE), :] = (dot_nt(pick, c_ref[...]) * slot_gate).astype(BF16)
        mine = rows_of(me.block(me.x, me.y, bi))
        here = pl.ds(mul((bi * 16 + me.p) * SLOT, 8), SLOT)
        recv_x[mine, :] = send_x[here, :]
        recv_g[mine, :] = send_g[here, :]

        @pl.loop(1, 16)
        def _(i):
            for cp in dispatch_copy(bi, i, False):
                cp.start()

    widen(tok, tok_in, True)
    widen(cot, cot_in, False)
    dispatch(0, meta, tok, cot)
    for cp in zex:
        cp.wait_recv()
    widen(tok, ztok, True)
    widen(cot, zcot, False)
    dispatch(1, zmeta, tok, cot)

    def forward_neighbours(a):
        ag_in(a, 0).wait_recv()
        ag(a, 3).start()
        ag(a, 5).start()
        ag_in(a, 1).wait_recv()
        ag(a, 4).start()
        ag(a, 6).start()

    forward_neighbours(3)
    forward_neighbours(0)
    forward_neighbours(1)
    for k in (0, 1, 2):
        ag(2, k).start()

    for bi in range(2):

        @pl.loop(1, 16)
        def _(i):
            for cp in dispatch_copy(bi, i, True):
                cp.wait_recv()

    eye_lane = one_zero(lax.broadcasted_iota(jnp.int32, (8, 128), 1) == OWN - 128).astype(BF16)
    flags = dot_nt(eye_lane, recv_x[:, 128:256])
    before = one_zero(
        lax.broadcasted_iota(jnp.int32, (SLOTS, SLOTS), 0) < lax.broadcasted_iota(jnp.int32, (SLOTS, SLOTS), 1)
    ).astype(BF16)
    position = dot(flags.astype(BF16), before)
    position = jnp.where(flags > 0.5, position, -1.0)[0:1, :]

    @pl.loop(0, 2)
    def _(m):
        at = mul(m * 256, 256)
        row = (lax.broadcasted_iota(jnp.int32, (256, SLOTS), 0) + at).astype(F32)
        pick = one_zero(row == position).astype(BF16)
        r_mat[pl.ds(at, 256), :] = pick
        x[pl.ds(at, 256), :] = dot(pick, recv_x[...]).astype(BF16)
        g[pl.ds(at, 256), :] = dot(pick, recv_g[...]).astype(BF16)

    def project(j, first):
        cols = pl.ds(mul(j * PAIR, 128), PAIR)
        live = lax.broadcasted_iota(jnp.int32, (SENT + 8, 128), 0) < OWN
        live = live & (lax.broadcasted_iota(jnp.int32, (SENT + 8, 128), 1) < REST)
        for core in range(2):
            misc = wrem[misc_at(j, core), :].astype(F32)
            rest = misc[: SENT + 8]
            for a in range(3):
                own = rest if a == 0 else pltpu.roll(rest, 128 - REST * a, 1)
                weights[a][rows_at(j, core, 0, SENT + 8), MAIN:] = jnp.where(live, own, 0.0).astype(BF16)
                for t in range(TILES):
                    at = OWN + TAIL * (a * TILES + t)
                    last = jnp.concatenate([misc[at : at + TAIL], jnp.zeros((8 - TAIL, 128), F32)], axis=0)
                    weights[a][rows_at(j, core, SENT, 8), 128 * t : 128 * (t + 1)] = last.astype(BF16)

        @pl.loop(0, 2)
        def _(m):
            rows = pl.ds(mul(m * 256, 256), 256)
            xs = x[rows, cols]
            for acc, w in ((acc_g, wg), (acc_u, wu)):
                part = dot(xs, w[cols, :])
                acc[rows, :] = part if first else acc[rows, :] + part

    for a in (3, 0, 1):
        ag_in(a, 2).wait_recv()
    project(h, True)
    for a in (3, 0, 1):
        ag_in(a, 5).wait_recv()
    project(up_j(3), False)
    for a in (3, 0, 1):
        ag_in(a, 6).wait_recv()
    project(up_j(1), False)

    def finish_gather(a):
        ag_in(a, 3).wait_recv()
        ag(a, 7).start()
        ag_in(a, 4).wait_recv()
        ag(a, 8).start()

    def wait_opposite(a):
        ag_in(a, 7).wait_recv()
        ag_in(a, 8).wait_recv()

    for a in (3, 0, 1):
        finish_gather(a)
    for a in (3, 0, 1):
        wait_opposite(a)
    project(up_j(2), False)

    @pl.loop(0, 16)
    def _(m):
        rows = pl.ds(mul(m * 32, 32), 32)
        gate, up = acc_g[rows, :], acc_u[rows, :] + 1.0
        sg = jax.nn.sigmoid(SWISH_SLOPE * gate)
        value = gate * sg
        slope = sg + SWISH_SLOPE * value * (1.0 - sg)
        hid[rows, :] = (value * up).astype(BF16)
        acc_g[rows, :] = up * slope
        acc_u[rows, :] = value

    arrays = ((pd, g, hid), (wg, x, dg), (wu, x, du), (grem, None, None))

    def ra(a, k):
        if a in (0, 3):
            return (ra_d if a == 0 else ra_rem).at[k]
        return (recv_x, recv_g)[a - 1].at[pl.ds(CHUNK * k, SENT), width(a)]

    def half_in(a, k):
        rows = pl.ds(*span(a, k))
        return hr.at[a, rows, :] if a < 3 else hr_rem.at[rows, :]

    def full_in(a, k):
        return fr.at[a * 2 + k] if a < 3 else fr_rem.at[k]

    def exchange(a, k):
        return remote(
            shard(a, arrays[a][0], up_j(k), 1 - c), ra(a, k), d2s.at[a * 4 + k], d2r.at[a * 4 + k], me.sibling
        )

    def parts_of(a, ks):
        parts, left, right = arrays[a]
        for k in ks:
            cols = pl.ds(mul(up_j(k) * PAIR, 128), PAIR)
            part = dot_tn(left[:, cols], right[...])
            parts[cols, :MAIN] = part[:, :MAIN].astype(BF16)
            exchange(a, k).start()
            for core in range(2):
                own = part[CHUNK * core : CHUNK * core + OWN]
                rest = own[:, MAIN:] if a == 0 else pltpu.roll(own[:, MAIN:], REST * a, 1)
                pieces = [rest]
                if a > 0:
                    pieces.append(jnp.zeros((a * TILES * TAIL, 128), F32))
                pieces += [own[SENT:, 128 * t : 128 * (t + 1)] for t in range(TILES)]
                if a < 2:
                    pieces.append(jnp.zeros(((2 - a) * TILES * TAIL, 128), F32))
                misc = jnp.concatenate(pieces, axis=0)
                at = misc_at(up_j(k), core)
                if a > 0:
                    misc = misc + grem[at, :].astype(F32)
                grem[at, :] = misc.astype(BF16)
            if a == 2:
                exchange(3, k).start()

    def half(a, k):
        return remote(
            shard(a, arrays[a][0], up_j(2), c, k),
            half_in(a, k),
            hss.at[a * 2 + k],
            hsr.at[a * 2 + k],
            (me.up, me.down)[k],
        )

    def full(a, k):
        return remote(
            shard(a, arrays[a][0], up_j((1, 3)[k]), c),
            full_in(a, k),
            fss.at[a * 2 + k],
            fsr.at[a * 2 + k],
            (me.up, me.down)[k],
        )

    def send_halves(a):
        exchange(a, 2).wait_recv()
        at = place_of(a, up_j(2), c)
        parts = arrays[a][0]
        parts[at] = (parts[at].astype(F32) + ra(a, 2)[...].astype(F32)).astype(BF16)
        half(a, 0).start()
        half(a, 1).start()

    def send_fulls(a):
        parts = arrays[a][0]
        for k, jj in ((0, 1), (1, 3)):
            exchange(a, jj).wait_recv()
            half(a, k).wait_recv()
            for with_half in (True, False):
                side = k if with_half else 1 - k
                at = place_of(a, up_j(jj), c, side)
                total = parts[at].astype(F32) + ra(a, jj)[pl.ds(*span(a, side)), :].astype(F32)
                if with_half:
                    total = total + half_in(a, k)[...].astype(F32)
                parts[at] = total.astype(BF16)
            full(a, k).start()

    def down_step(j, first):
        cols = pl.ds(mul(j * PAIR, 128), PAIR)

        @pl.loop(0, 2)
        def _(m):
            rows = pl.ds(mul(m * 256, 256), 256)
            part = dot(g[rows, cols], wd[cols, :])
            acc_d[rows, :] = part if first else acc_d[rows, :] + part

    def out_step(j):
        cols = pl.ds(mul(j * PAIR, 128), PAIR)

        @pl.loop(0, 2)
        def _(m):
            rows = pl.ds(mul(m * 256, 256), 256)
            eo[rows, cols] = dot_nt(hid[rows, :], wd[cols, :]).astype(BF16)

    parts_of(0, (2, 1, 3, 0))
    for cp in zex:
        cp.wait_send()
    for bi in range(2):

        @pl.loop(1, 16)
        def _(i):
            for cp in dispatch_copy(bi, i, False):
                cp.wait_send()

    for a in (3, 0, 1):
        for k in range(9):
            ag(a, k).wait_send()
    forward_neighbours(2)
    send_halves(0)
    ag_in(2, 2).wait_recv()
    down_step(h, True)
    out_step(h)
    ag_in(2, 5).wait_recv()
    down_step(up_j(3), False)
    ag_in(2, 6).wait_recv()
    down_step(up_j(1), False)
    finish_gather(2)
    wait_opposite(2)
    down_step(up_j(2), False)

    @pl.loop(0, 16)
    def _(m):
        rows = pl.ds(mul(m * 32, 32), 32)
        dh = acc_d[rows, :]
        dg[rows, :] = (dh * acc_g[rows, :]).astype(BF16)
        du[rows, :] = (dh * acc_u[rows, :]).astype(BF16)

    parts_of(1, (2, 1))
    send_halves(1)
    parts_of(1, (3, 0))
    parts_of(2, (2, 1))
    send_halves(2)
    send_halves(3)
    send_fulls(0)
    parts_of(2, (3, 0))
    for k in (3, 1, 2):
        out_step(up_j(k))

    def back_copy(bi, i, incoming):
        p, px, py = me.plane(i, -1 if incoming else 1)
        place = p if incoming else me.p
        k = bi * 16 + i
        return remote(
            rets.at[rows_of(me.block(px, py, bi)), :],
            rr.at[pl.ds(mul((bi * 16 + place) * SLOT, 8), SLOT), :],
            rs.at[k],
            rr_sem.at[k],
            me.plane_device(px, py),
        )

    @pl.loop(0, 2)
    def _(m):
        cols = pl.ds(mul(m * PLANE, 128), PLANE)
        rets[pl.ds(mul(m * PLANE, 8), PLANE), :] = dot_tn(r_mat[:, cols], eo[...]).astype(BF16)

    send_fulls(1)
    for bi in range(2):
        rr[pl.ds(mul((bi * 16 + me.p) * SLOT, 8), SLOT), :] = rets[rows_of(me.block(me.x, me.y, bi)), :]

        @pl.loop(1, 16)
        def _(i):
            back_copy(bi, i, False).start()

    send_fulls(2)
    send_fulls(3)

    for bi in range(2):

        @pl.loop(1, 16)
        def _(i):
            back_copy(bi, i, True).wait_recv()

    def combine(bi):
        weight = mt[bi]
        high = weight.astype(BF16)
        low = (weight - high.astype(F32)).astype(BF16)
        both = dot_tn(rr[pl.ds(bi * PLANE, PLANE), :], jnp.concatenate([high, low], axis=1))
        return both[:, :TOK] + both[:, TOK:]

    theirs = combine(1).astype(BF16)
    for k in range(8):
        zsend[OWN * k : OWN * (k + 1), :] = theirs[CHUNK * k : CHUNK * k + OWN, :]
    zcopy = remote(zsend, zrecv, zs.at[3], zr.at[3], me.partner)
    zcopy.start()
    own = combine(0)
    zcopy.wait_recv()
    for k in range(8):
        at = slice(OWN * k, OWN * (k + 1))
        mixed_out[at, :] = (own[CHUNK * k : CHUNK * k + OWN, :] + zrecv[at, :].astype(F32)).astype(BF16)

    for k in range(9):
        ag(2, k).wait_send()
    for a in range(4):
        for k in range(4):
            exchange(a, k).wait_send()
        for k in range(2):
            half(a, k).wait_send()
    for bi in range(2):

        @pl.loop(1, 16)
        def _(i):
            back_copy(bi, i, False).wait_send()

    for a in range(4):
        exchange(a, 0).wait_recv()
        total = arrays[a][0][place_of(a, h, c)].astype(F32) + ra(a, 0)[...].astype(F32)
        for k in range(2):
            full(a, k).wait_recv()
            total = total + full_in(a, k)[...].astype(F32)
        if a < 3:
            outs[a][:SENT, :MAIN] = total.astype(BF16)
        else:
            for b in range(3):
                own = total[:OWN] if b == 0 else pltpu.roll(total[:OWN], 128 - REST * b, 1)
                outs[b][:, MAIN:] = own.astype(BF16)[:, :REST]
                for t in range(TILES):
                    at = OWN + TAIL * (b * TILES + t)
                    outs[b][SENT:, 128 * t : 128 * (t + 1)] = total[at : at + TAIL].astype(BF16)

    zcopy.wait_send()
    for a in range(4):
        for k in range(2):
            full(a, k).wait_send()


def copy_kernel(*refs):
    srcs, dsts, held, (sem_in, sem_out) = refs[:4], refs[4:8], refs[8:12], refs[12:]
    loads = [pltpu.make_async_copy(s, v, sem_in.at[i]) for i, (s, v) in enumerate(zip(srcs, held))]
    stores = [pltpu.make_async_copy(v, d, sem_out.at[i]) for i, (v, d) in enumerate(zip(held, dsts))]
    for load in loads:
        load.start()
    for load, store in zip(loads, stores):
        load.wait()
        store.start()
    for store in stores:
        store.wait()


def body(tokens, cotangent, expert_ids, gate_weights, w_gate, w_up, w_down):
    dma = pltpu.SemaphoreType.DMA
    b16 = lambda *shape: pltpu.VMEM(shape, BF16)
    f32 = lambda *shape: pltpu.VMEM(shape, F32)
    results = [jax.ShapeDtypeStruct((OWN, FH), BF16)] * 3 + [jax.ShapeDtypeStruct((D, TOK), BF16)]
    anywhere = pl.BlockSpec(memory_space=pl.ANY)
    outs = pl.pallas_call(
        step_kernel,
        name="step",
        out_shape=results,
        in_specs=[anywhere] * 7,
        out_specs=[VM()] * 4,
        scratch_shapes=[
            pltpu.VMEM((4, TOK), jnp.int32), f32(4, TOK), b16(D, TOK), b16(D, TOK),
            b16(DP, DP), b16(DP, DP), b16(DP, DP), b16(8 * MISC, 128), b16(8 * MISC, 128),
            b16(4, MISC, 128), b16(MISC, 128), b16(2, MISC, 128),
            f32(8, TOK), f32(8, TOK), b16(DP, TOK), b16(DP, TOK), b16(D, TOK), b16(D, TOK),
            b16(SLOTS, DP), b16(SLOTS, DP), b16(SLOTS, DP), b16(SLOTS, DP),
            b16(CAP, DP), b16(CAP, DP), b16(CAP, DP), b16(CAP, DP),
            f32(CAP, DP), f32(CAP, DP), f32(CAP, DP),
            b16(DP, DP), b16(4, SENT, MAIN), b16(3, SENT, MAIN), b16(6, SENT, MAIN),
            b16(SLOTS, DP), b16(SLOTS, DP), b16(CAP, SLOTS), f32(2, PLANE, TOK), b16(D, TOK), b16(D, TOK),
            dma((7,)), dma((4,)), dma((4,)), dma((36,)), dma((36,)), dma((64,)), dma((64,)),
            dma((16,)), dma((16,)), dma((8,)), dma((8,)), dma((8,)), dma((8,)), dma((32,)), dma((32,)),
        ],
        compiler_params=pltpu.CompilerParams(
            collective_id=0, has_side_effects=True, vmem_limit_bytes=67043328
        ),
    )(expert_ids.T, gate_weights.T, tokens.T, cotangent.T, w_gate, w_up, w_down)
    gg, gu, gd, mixed = pl.pallas_call(
        copy_kernel,
        name="results",
        out_shape=results,
        in_specs=[anywhere] * 4,
        out_specs=[anywhere] * 4,
        scratch_shapes=[b16(*r.shape) for r in results] + [dma((4,)), dma((4,))],
    )(*outs)
    return mixed.T, gg[None], gu[None], gd[None]


def solution(mesh):
    rows, weight = P(("expert", "dp"), None), P("expert", "dp", None)
    return jax.shard_map(
        body,
        mesh=mesh,
        in_specs=(rows, rows, rows, rows, weight, weight, weight),
        out_specs=(rows, weight, weight, weight),
        check_vma=False,
    )
```
